256 devices in a mesh: section: 4 (over y_hi, core), dp: 64 (over y_lo, x, z).
Axes of the slice: x: 4, y: 4 (y_hi: 2, y_lo: 2; y = y_hi * 2 + y_lo), z: 8, core: 2. Of those that a mesh axis runs over, the one named last changes fastest.
Arguments:
- latents: bfloat16 [128, 4, 128], P('dp'), may hold values from -6 to 6
- noise: bfloat16 [128, 4, 128], P('dp'), may hold values from -6 to 6
- timesteps: int32 [128], P('dp'), may hold values from 0 to 999
- cameras: int32 [128, 4], P('dp'), may hold values from 0 to 31
- embed_in: bfloat16 [4, 1024], replicated, may hold values from -3 to 3
- camera_table: bfloat16 [32, 1024], replicated, may hold values from -6 to 6
- w_mod: bfloat16 [4, 256, 3072], P('section'), may hold values from -0.375 to 0.375
- w_qkv: bfloat16 [4, 1024, 3072], P('section'), may hold values from -0.1875 to 0.1875
- w_out: bfloat16 [4, 1024, 1024], P('section'), may hold values from -0.1875 to 0.1875
- head_out: bfloat16 [4, 1024], replicated, may hold values from -0.1875 to 0.1875
- moment_qkv: float32 [4, 1024, 3072], P('section', 'dp'), may hold values from -6 to 6
- moment_out: float32 [4, 1024, 1024], P('section', 'dp'), may hold values from -6 to 6
- second_qkv: float32 [4, 1024, 3072], P('section', 'dp'), may hold values from 0.25 to 4
- second_out: float32 [4, 1024, 1024], P('section', 'dp'), may hold values from 0.25 to 4
Outputs:
- update_qkv: float32 [4, 1024, 3072], P('section', 'dp')
- update_out: float32 [4, 1024, 1024], P('section', 'dp')
- new_moment_qkv: float32 [4, 1024, 3072], P('section', 'dp')
- new_moment_out: float32 [4, 1024, 1024], P('section', 'dp')
- new_second_qkv: float32 [4, 1024, 3072], P('section', 'dp')
- new_second_out: float32 [4, 1024, 1024], P('section', 'dp')
The draws below stay inside these ranges and needn't reach their ends.
All inputs are finite; a program needn't handle non-finite values.
Results may differ from the reference program's by a relative error of at most 0.00045.
Values may be sent and summed in bfloat16 or wider, within the bound.
A program may use at most 128 MiB of HBM per device.

```python
import math
import jax
import jax.numpy as jnp
from jax import lax

D = 1024
HEADS = 16
HEAD_DIM = 64
CH = 4
TEMB = 256
CAMERAS = 32
VIEWS = 4
SEQ = 128
SAMPLES = 128
LAYERS = 4


def set_ends(entries, own_key, least, high):
    index_at = [jax.random.randint(jax.random.fold_in(own_key, axis), (), 0, length) for axis, length in enumerate(entries.shape)]
    longest = entries.shape.index(max(entries.shape))
    next_to = index_at[:longest] + [(index_at[longest] + 1) % entries.shape[longest]] + index_at[longest + 1:]
    return entries.at[tuple(index_at)].set(least).at[tuple(next_to)].set(high)


def steps_of(stream_key, dims, cuts, least, largest):
    loudness, own = 1.0, jax.random.fold_in(stream_key, 6)
    for axis_at, blocks in cuts:
        heights = jnp.exp(jax.random.uniform(jax.random.fold_in(own, axis_at), (blocks,), jnp.float32, least / len(cuts), largest / len(cuts)))
        loudness = loudness * jnp.repeat(heights, dims[axis_at] // blocks).reshape([-1 if axis == axis_at else 1 for axis in range(len(dims))])
    return loudness


def centred(rng, dims, scale, reach, pieces=(), held_as=jnp.bfloat16):
    drawn = jax.random.normal(rng, dims, jnp.float32) * scale
    if len(pieces) > 0:
        drawn = steps_of(rng, dims, pieces, -0.22, 0.18) * drawn
    return jnp.clip(drawn, min=-reach, max=reach).astype(held_as)


def setup_inputs(seed: int = 0) -> dict:
    streams_of = jax.random.split(jax.random.key(seed), 15)
    latents = centred(streams_of[0], (SAMPLES, CH, SEQ), 1.0, 6.0, ((0, 64),))
    noise = centred(streams_of[1], (SAMPLES, CH, SEQ), 1.0, 6.0, ((0, 64),))
    timesteps = set_ends(jax.random.randint(streams_of[2], (SAMPLES,), 0, 1000), jax.random.fold_in(streams_of[2], 1), 0, 999).astype(jnp.int32)
    cameras = set_ends(jax.random.randint(streams_of[3], (SAMPLES, VIEWS), 0, CAMERAS), jax.random.fold_in(streams_of[3], 1), 0, CAMERAS - 1).astype(jnp.int32)
    embed_in = centred(streams_of[4], (CH, D), CH ** -0.5, 3.0)
    camera_table = centred(streams_of[5], (CAMERAS, D), 1.0, 6.0)
    w_mod = centred(streams_of[6], (LAYERS, TEMB, 3 * D), TEMB ** -0.5, 0.375, ((0, 4),))
    w_qkv = centred(streams_of[7], (LAYERS, D, 3 * D), D ** -0.5, 0.1875, ((0, 4),))
    w_out = centred(streams_of[8], (LAYERS, D, D), D ** -0.5, 0.1875, ((0, 4),))
    head_out = centred(streams_of[9], (CH, D), D ** -0.5, 0.1875)
    moment_qkv = centred(streams_of[10], (LAYERS, D, 3 * D), 1.0, 6.0, ((0, 4), (1, 64)), jnp.float32)
    moment_out = centred(streams_of[11], (LAYERS, D, D), 1.0, 6.0, ((0, 4), (1, 64)), jnp.float32)
    second_qkv = jnp.clip(jnp.exp(math.log(4.0) - 2.7725887 * jax.random.uniform(streams_of[12], (LAYERS, D, 3 * D), jnp.float32) ** steps_of(streams_of[12], (LAYERS, D, 3 * D), ((0, 4), (1, 64)), -0.2, 0.2)), 0.25, 4.0)
    second_out = jnp.clip(jnp.exp(math.log(4.0) - 2.7725887 * jax.random.uniform(streams_of[13], (LAYERS, D, D), jnp.float32) ** steps_of(streams_of[13], (LAYERS, D, D), ((0, 4), (1, 64)), -0.2, 0.2)), 0.25, 4.0)
    return {"latents": latents, "noise": noise, "timesteps": timesteps, "cameras": cameras, "embed_in": embed_in, "camera_table": camera_table, "w_mod": w_mod, "w_qkv": w_qkv, "w_out": w_out, "head_out": head_out, "moment_qkv": moment_qkv, "moment_out": moment_out, "second_qkv": second_qkv, "second_out": second_out}


def time_embed(step_ids, emb_width):
    half_dim = emb_width // 2
    frequency = jnp.exp(-math.log(10000.0) * jnp.arange(half_dim, dtype=jnp.float32) / half_dim)
    phases = step_ids.astype(jnp.float32)[:, None] * frequency[None, :]
    joined = jnp.concatenate([jnp.cos(phases), jnp.sin(phases)], axis=-1)
    return jax.nn.silu(joined).astype(jnp.bfloat16)

def embed_sample(latent_now, noise_now, step_now, camera_now, embed_in, camera_table):
    step_f = step_now.astype(jnp.float32)
    alpha_bar = jnp.cos((step_f / 1000.0 + 0.008) / 1.008 * (math.pi / 2.0)) ** 2
    noised = jnp.sqrt(alpha_bar) * latent_now.astype(jnp.float32) + jnp.sqrt(1.0 - alpha_bar) * noise_now.astype(jnp.float32)
    features = lax.dot_general(noised.astype(jnp.bfloat16), embed_in, (((0,), (0,)), ((), ())), preferred_element_type=jnp.float32)
    onehot = (camera_now[:, None] == jnp.arange(camera_table.shape[0], dtype=jnp.int32)[None, :]).astype(jnp.bfloat16)
    camera_vec = jnp.dot(onehot, camera_table, preferred_element_type=jnp.float32)
    model_width = embed_in.shape[1]
    views = camera_now.shape[0]
    joined = features.reshape(views, -1, model_width) + camera_vec[:, None, :]
    return joined.reshape(-1, model_width).astype(jnp.bfloat16)

def normed_of(layer_h, shift_mod, scale_mod):
    hidden_f = layer_h.astype(jnp.float32)
    mean_sq = lax.optimization_barrier(jnp.mean(hidden_f * hidden_f, axis=-1, keepdims=True))
    return (hidden_f * lax.rsqrt(mean_sq + 1e-06) * (1.0 + scale_mod) + shift_mod).astype(jnp.bfloat16)

def piece_a(layer_h, weight_qkv, shift_mod, scale_mod):
    normed = normed_of(layer_h, shift_mod, scale_mod)
    return jnp.dot(normed, weight_qkv, preferred_element_type=jnp.float32).astype(jnp.bfloat16)

def piece_b(qkv_rows):
    seq_len = qkv_rows.shape[0]
    model_width = qkv_rows.shape[1] // 3
    queries = qkv_rows[:, :model_width].reshape(seq_len, HEADS, HEAD_DIM).astype(jnp.float32)
    keys_in = qkv_rows[:, model_width:2 * model_width].reshape(seq_len, HEADS, HEAD_DIM).astype(jnp.float32)
    values_in = qkv_rows[:, 2 * model_width:].reshape(seq_len, HEADS, HEAD_DIM).astype(jnp.float32)
    scores = jnp.einsum('qhd,khd->hqk', queries, keys_in) * (1.0 / math.sqrt(HEAD_DIM))
    probabilities = jax.nn.softmax(scores, axis=-1).astype(jnp.bfloat16)
    attended = jnp.einsum('hqk,khd->qhd', probabilities.astype(jnp.float32), values_in)
    return attended.reshape(seq_len, model_width).astype(jnp.bfloat16)

def piece_c(attended, layer_h, weight_out, gate_mod):
    projected = jnp.dot(attended, weight_out, preferred_element_type=jnp.float32)
    return (layer_h.astype(jnp.float32) + gate_mod * projected).astype(jnp.bfloat16)

def output_grad(final_h, head_out, noise_now):

    def squared(hidden_in):
        hidden_f = hidden_in.astype(jnp.float32)
        mean_sq = lax.optimization_barrier(jnp.mean(hidden_f * hidden_f, axis=-1, keepdims=True))
        normed = (hidden_f * lax.rsqrt(mean_sq + 1e-06)).astype(jnp.bfloat16)
        predicted = lax.dot_general(head_out, normed, (((1,), (1,)), ((), ())), preferred_element_type=jnp.float32)
        error_val = predicted - noise_now.astype(jnp.float32)
        return jnp.sum(error_val * error_val)
    loss_val, pull_back = jax.vjp(squared, final_h)
    return pull_back(jnp.ones_like(loss_val))[0]

def layer_backward(grad_out, layer_h, qkv_rows, attended, weight_qkv, weight_out, shift_mod, scale_mod, gate_mod):
    _, pull_c = jax.vjp(lambda attn_in, hidden_in: piece_c(attn_in, hidden_in, weight_out, gate_mod), attended, layer_h)
    grad_attn, grad_res = pull_c(grad_out)
    proj_cot = (gate_mod * grad_out.astype(jnp.float32)).astype(jnp.bfloat16)
    grad_wout = lax.dot_general(attended, proj_cot, (((0,), (0,)), ((), ())), preferred_element_type=jnp.float32)
    _, pull_b = jax.vjp(piece_b, qkv_rows)
    grad_qkv_rows = pull_b(grad_attn)[0]
    _, pull_a = jax.vjp(lambda hidden_in: piece_a(hidden_in, weight_qkv, shift_mod, scale_mod), layer_h)
    grad_hidden = pull_a(grad_qkv_rows)[0]
    normed = normed_of(layer_h, shift_mod, scale_mod)
    grad_wqkv = lax.dot_general(normed, grad_qkv_rows, (((0,), (0,)), ((), ())), preferred_element_type=jnp.float32)
    grad_total = (grad_hidden.astype(jnp.float32) + grad_res.astype(jnp.float32)).astype(jnp.bfloat16)
    return (grad_total, grad_wqkv, grad_wout)

def optimizer_step(gradient, moment, second, factor):
    normalized = gradient * factor
    moment_new = 0.9 * moment + 0.1 * normalized
    second_new = 0.99 * second + 0.01 * normalized * normalized
    return (moment_new / (jnp.sqrt(second_new) + 1e-08), moment_new, second_new)

def reference(latents, noise, timesteps, cameras, embed_in, camera_table, w_mod, w_qkv, w_out, head_out, moment_qkv, moment_out, second_qkv, second_out):
    model_width = w_qkv.shape[1]
    time_emb = time_embed(timesteps, w_mod.shape[1])

    def per_sample(carried, sample_item):
        latent_now, noise_now, emb_now, camera_now, step_now = sample_item
        layer_h = embed_sample(latent_now, noise_now, step_now, camera_now, embed_in, camera_table)
        stored = []
        for layer_num in range(LAYERS):
            modulation = jnp.dot(emb_now[None, :], w_mod[layer_num], preferred_element_type=jnp.float32)[0]
            shift_mod = modulation[:model_width]
            scale_mod = modulation[model_width:2 * model_width]
            gate_mod = modulation[2 * model_width:]
            qkv_rows = piece_a(layer_h, w_qkv[layer_num], shift_mod, scale_mod)
            attended = piece_b(qkv_rows)
            stored.append((layer_h, qkv_rows, attended, shift_mod, scale_mod, gate_mod))
            layer_h = piece_c(attended, layer_h, w_out[layer_num], gate_mod)
        grad_h = output_grad(layer_h, head_out, noise_now)
        grads_qkv = [None] * LAYERS
        grads_out = [None] * LAYERS
        for layer_num in reversed(range(LAYERS)):
            saved_h, qkv_rows, attended, shift_mod, scale_mod, gate_mod = stored[layer_num]
            grad_h, grads_qkv[layer_num], grads_out[layer_num] = layer_backward(grad_h, saved_h, qkv_rows, attended, w_qkv[layer_num], w_out[layer_num], shift_mod, scale_mod, gate_mod)
        return ((carried[0] + jnp.stack(grads_qkv), carried[1] + jnp.stack(grads_out)), None)
    start = (jnp.zeros(w_qkv.shape, jnp.float32), jnp.zeros(w_out.shape, jnp.float32))
    (grad_qkv, grad_out), _ = lax.scan(per_sample, start, (latents, noise, time_emb, cameras, timesteps))
    total_sq = jnp.sum(grad_qkv * grad_qkv) + jnp.sum(grad_out * grad_out)
    factor = lax.rsqrt(total_sq / (LAYERS * 4 * model_width * model_width) + 1e-12)
    update_qkv, new_moment_qkv, new_second_qkv = optimizer_step(grad_qkv, moment_qkv, second_qkv, factor)
    update_out, new_moment_out, new_second_out = optimizer_step(grad_out, moment_out, second_out, factor)
    return (update_qkv, update_out, new_moment_qkv, new_moment_out, new_second_qkv, new_second_out)
```

```python
import functools
import math

import jax
import jax.numpy as jnp
from jax import lax
from jax.experimental import pallas as pl
from jax.experimental.pallas import tpu as pltpu
from jax.sharding import Mesh
from jax.sharding import PartitionSpec as P

HEADS = 16
HEAD_DIM = 64
SECTION = ("section_0", "section_1")
DP = ("dp_0", "dp_1", "dp_2")
MESH = pl.DeviceIdType.MESH
F32 = jnp.float32
BF16 = jnp.bfloat16
D = 1024
SEQ = 128
NX = 4
NZ = 8
QB = 3 * D // NX
OB = D // NX
VMEM = pl.BlockSpec(memory_space=pltpu.VMEM)


def time_embed(step_ids, emb_width):
    half_dim = emb_width // 2
    frequency = jnp.exp(-math.log(10000.0) * jnp.arange(half_dim, dtype=jnp.float32) / half_dim)
    phases = step_ids.astype(jnp.float32)[:, None] * frequency[None, :]
    joined = jnp.concatenate([jnp.cos(phases), jnp.sin(phases)], axis=-1)
    return jax.nn.silu(joined).astype(jnp.bfloat16)


def embed_sample(latent_now, noise_now, step_now, camera_now, embed_in, camera_table):
    step_f = step_now.astype(jnp.float32)
    alpha_bar = jnp.cos((step_f / 1000.0 + 0.008) / 1.008 * (math.pi / 2.0)) ** 2
    noised = jnp.sqrt(alpha_bar) * latent_now.astype(jnp.float32) + jnp.sqrt(
        1.0 - alpha_bar
    ) * noise_now.astype(jnp.float32)
    features = lax.dot_general(
        noised.astype(jnp.bfloat16),
        embed_in,
        (((0,), (0,)), ((), ())),
        preferred_element_type=jnp.float32,
    )
    onehot = (
        camera_now[:, None] == jnp.arange(camera_table.shape[0], dtype=jnp.int32)[None, :]
    ).astype(jnp.bfloat16)
    camera_vec = jnp.dot(onehot, camera_table, preferred_element_type=jnp.float32)
    model_width = embed_in.shape[1]
    views = camera_now.shape[0]
    joined = features.reshape(views, -1, model_width) + camera_vec[:, None, :]
    return joined.reshape(-1, model_width).astype(jnp.bfloat16)


def dot_nn(a, b):
    return lax.dot_general(a, b, (((1,), (0,)), ((), ())), preferred_element_type=F32)


def dot_nt(a, b):
    return lax.dot_general(a, b, (((1,), (1,)), ((), ())), preferred_element_type=F32)


def dot_tn(a, b):
    return lax.dot_general(a, b, (((0,), (0,)), ((), ())), preferred_element_type=F32)


def lanes(start, size):
    return pl.ds(pl.multiple_of(start, 128), size)


def pipe_kernel(
    h0_ref, mod_ref, noise_ref, wqkv_ref, wout_ref, head_ref,
    nall, aall, ball, pall,
    h_scr, hn_scr, nrm_scr, att_scr, qkv_scr, p_scr, r_scr, g_scr, gs_scr,
    dqkv_scr, pc_scr, datt_scr, tmp_scr, mods, noi,
    h_send, h_recv, g_send, g_recv, sw_send, sw_recv, x_send, x_recv,
):
    s0 = lax.axis_index("section_0")
    s1 = lax.axis_index("section_1")
    d0 = lax.axis_index("dp_0")
    mx = lax.axis_index("dp_1")
    sec = 2 * s0 + s1

    def toward(step):
        other = sec + step
        o0 = lax.rem(lax.div(other + 4, 2), 2)
        o1 = lax.rem(other + 4, 2)
        crossing = (o0 + s0) - 2 * o0 * s0
        od = (d0 + crossing) - 2 * d0 * crossing
        return {"section_0": o0, "section_1": o1, "dp_0": od}

    nxt = toward(1)
    prv = toward(-1)
    partner = {"dp_0": 1 - d0}

    barrier = pltpu.get_barrier_semaphore()

    def greet(where):
        pl.semaphore_signal(barrier, inc=1, device_id=where, device_id_type=MESH)

    for d in range(1, NX):
        greet({"dp_1": lax.rem(mx + d, NX)})

    @pl.when(sec < 3)
    def _():
        greet(nxt)

    @pl.when(sec > 0)
    def _():
        greet(prv)

    @pl.when(s0 == 1)
    def _():
        greet(partner)

    pl.semaphore_wait(barrier, NX - 1 + lax.min(sec, 1) + lax.min(3 - sec, 1) + s0)

    def remote(src, dst, ssem, rsem, where):
        return pltpu.make_async_remote_copy(
            src_ref=src, dst_ref=dst, send_sem=ssem, recv_sem=rsem,
            device_id=where, device_id_type=MESH,
        )

    def swap_mod():
        return remote(mod_ref, mods, sw_send.at[0], sw_recv.at[0], partner)

    def swap_noise():
        return remote(noise_ref, noi, sw_send.at[1], sw_recv.at[1], partner)

    @pl.when(s0 == 1)
    def _():
        swap_mod().start()
        swap_noise().start()
        swap_mod().wait_recv()
        swap_noise().wait_recv()

    @pl.when(s0 == 0)
    def _():
        mods[...] = mod_ref[...]

    def h_copy(m):
        return remote(hn_scr.at[m], h_scr.at[m], h_send.at[m], h_recv.at[m], nxt)

    def g_copy(m):
        return remote(gs_scr.at[m], g_scr.at[m], g_send.at[m], g_recv.at[m], prv)

    def x_copies(m, which):
        rows = pl.ds(m * SEQ, SEQ)
        made = []
        for d in range(1, NX):
            to = lax.rem(mx + d, NX)
            where = {"dp_1": to}
            for k in which:
                src, dst = (
                    (nrm_scr.at[m], nall.at[mx, rows]),
                    (att_scr.at[m], aall.at[mx, rows]),
                    (dqkv_scr.at[m, :, lanes(to * QB, QB)], ball.at[mx, rows]),
                    (pc_scr.at[m, :, lanes(to * OB, OB)], pall.at[mx, rows]),
                )[k]
                made.append(remote(src, dst, x_send.at[m, d - 1, k], x_recv.at[m, d - 1, k], where))
        return made

    low = lax.broadcasted_iota(jnp.int32, (SEQ, 128), 1) < HEAD_DIM

    def both(tile):
        zero = jnp.zeros_like(tile)
        return jnp.concatenate([jnp.where(low, tile, zero), jnp.where(low, zero, tile)], axis=0)

    def merged(pair):
        return jnp.where(low, pair[:SEQ], pair[SEQ:])

    PAIRS = HEADS // 2
    GROUP = 4

    def over_pairs(body):
        def step(i, carry):
            for j in range(GROUP):
                body(i * GROUP + j)
            return carry

        lax.fori_loop(0, PAIRS // GROUP, step, 0)

    def forward(m, carry):
        @pl.when(sec == 0)
        def _():
            h_scr[m] = h0_ref[m]

        @pl.when(sec > 0)
        def _():
            h_copy(m).wait_recv()

        shift = mods[pl.ds(m * 8, 1), :]
        scale = mods[pl.ds(m * 8 + 1, 1), :]
        gate = mods[pl.ds(m * 8 + 2, 1), :]
        hf = h_scr[m].astype(F32)
        r = lax.rsqrt(jnp.mean(hf * hf, axis=-1, keepdims=True) + 1e-06)
        r_scr[m] = jnp.broadcast_to(r, (SEQ, 128))
        nrm_scr[m] = (hf * r * (1.0 + scale) + shift).astype(BF16)
        for n in range(6):
            cols = pl.ds(n * 512, 512)
            qkv_scr[m, :, cols] = dot_nn(nrm_scr[m], wqkv_ref[:, cols]).astype(BF16)

        def pair(j):
            q = qkv_scr[m, :, lanes(j * 128, 128)]
            k = qkv_scr[m, :, lanes(D + j * 128, 128)]
            v = qkv_scr[m, :, lanes(2 * D + j * 128, 128)]
            s = dot_nt(both(q), k) * (1.0 / math.sqrt(HEAD_DIM))
            s = jnp.exp(s - jnp.max(s, axis=-1, keepdims=True))
            p = s / jnp.sum(s, axis=-1, keepdims=True)
            p_scr[m, j] = p
            att_scr[m, :, lanes(j * 128, 128)] = merged(dot_nn(p.astype(BF16), v)).astype(BF16)

        over_pairs(pair)
        for n in range(2):
            cols = pl.ds(n * 512, 512)
            proj = dot_nn(att_scr[m], wout_ref[:, cols])
            hn_scr[m, :, cols] = (
                h_scr[m, :, cols].astype(F32) + gate[:, n * 512 : (n + 1) * 512] * proj
            ).astype(BF16)

        @pl.when(sec < 3)
        def _():
            h_copy(m).start()

        for copy in x_copies(m, (0, 1)):
            copy.start()
        rows = pl.ds(m * SEQ, SEQ)
        nall[mx, rows] = nrm_scr[m]
        aall[mx, rows] = att_scr[m]

        @pl.when(sec == 3)
        def _():
            ff = hn_scr[m].astype(F32)
            rr = lax.rsqrt(jnp.mean(ff * ff, axis=-1, keepdims=True) + 1e-06)
            predicted = dot_nt(head_ref[...], (ff * rr).astype(BF16))
            err = 2.0 * (predicted - noi[m])
            hi = err.astype(BF16)
            lo = (err - hi.astype(F32)).astype(BF16)
            dn = (dot_tn(hi, head_ref[...]) + dot_tn(lo, head_ref[...])).astype(BF16).astype(F32)
            inner = jnp.sum(dn * ff, axis=-1, keepdims=True) * (1.0 / D)
            g_scr[m] = (dn * rr - ff * (rr * rr * rr * inner)).astype(BF16)

        return carry

    lax.fori_loop(0, 2, forward, 0)

    def backward(m, carry):
        @pl.when(sec < 3)
        def _():
            g_copy(m).wait_recv()

        scale = mods[pl.ds(m * 8 + 1, 1), :]
        gate = mods[pl.ds(m * 8 + 2, 1), :]
        pc_scr[m] = (gate * g_scr[m].astype(F32)).astype(BF16)
        for copy in x_copies(m, (3,)):
            copy.start()
        for n in range(2):
            cols = pl.ds(n * 512, 512)
            datt_scr[:, cols] = dot_nt(pc_scr[m], wout_ref[cols, :]).astype(BF16)

        def pair(j):
            cq, ck, cv = lanes(j * 128, 128), lanes(D + j * 128, 128), lanes(2 * D + j * 128, 128)
            q2 = both(qkv_scr[m, :, cq])
            k = qkv_scr[m, :, ck]
            v = qkv_scr[m, :, cv]
            do2 = both(datt_scr[:, cq])
            p = p_scr[m, j]
            dv = dot_tn(p.astype(BF16), do2)
            dp = dot_nt(do2, v).astype(BF16).astype(F32)
            ds = p * (dp - jnp.sum(dp * p, axis=-1, keepdims=True))
            ds = (ds * (1.0 / math.sqrt(HEAD_DIM))).astype(BF16)
            dqkv_scr[m, :, cv] = dv.astype(BF16)
            dqkv_scr[m, :, cq] = merged(dot_nn(ds, k)).astype(BF16)
            dqkv_scr[m, :, ck] = dot_tn(ds, q2).astype(BF16)

        over_pairs(pair)
        for copy in x_copies(m, (2,)):
            copy.start()

        @pl.when(sec > 0)
        def _():
            for n in range(2):
                cols = pl.ds(n * 512, 512)
                tmp_scr[:, cols] = dot_nt(dqkv_scr[m], wqkv_ref[cols, :]).astype(BF16)
            hf = h_scr[m].astype(F32)
            r = r_scr[m][:, :1]
            u = tmp_scr[...].astype(F32) * (1.0 + scale)
            inner = jnp.sum(u * hf, axis=-1, keepdims=True) * (1.0 / D)
            dh = (u * r - hf * (r * r * r * inner)).astype(BF16).astype(F32)
            gs_scr[m] = (dh + g_scr[m].astype(F32)).astype(BF16)
            g_copy(m).start()

        rows = pl.ds(m * SEQ, SEQ)
        ball[mx, rows] = dqkv_scr[m, :, lanes(mx * QB, QB)]
        pall[mx, rows] = pc_scr[m, :, lanes(mx * OB, OB)]
        return carry

    lax.fori_loop(0, 2, backward, 0)

    def finish(m, carry):
        for copy in x_copies(m, (0, 1, 2, 3)):
            copy.wait()

        @pl.when(sec < 3)
        def _():
            h_copy(m).wait_send()

        @pl.when(sec > 0)
        def _():
            g_copy(m).wait_send()

        return carry

    lax.fori_loop(0, 2, finish, 0)

    @pl.when(s0 == 1)
    def _():
        swap_mod().wait_send()
        swap_noise().wait_send()


def run_pipe(h0, mod, noise, w_qkv, w_out, head):
    shape = jax.ShapeDtypeStruct
    dma = pltpu.SemaphoreType.DMA
    return pl.pallas_call(
        pipe_kernel,
        out_shape=(
            shape((NX, 2 * SEQ, D), BF16),
            shape((NX, 2 * SEQ, D), BF16),
            shape((NX, 2 * SEQ, QB), BF16),
            shape((NX, 2 * SEQ, OB), BF16),
        ),
        in_specs=[VMEM] * 6,
        out_specs=[VMEM] * 4,
        scratch_shapes=[
            pltpu.VMEM((2, SEQ, D), BF16),
            pltpu.VMEM((2, SEQ, D), BF16),
            pltpu.VMEM((2, SEQ, D), BF16),
            pltpu.VMEM((2, SEQ, D), BF16),
            pltpu.VMEM((2, SEQ, 3 * D), BF16),
            pltpu.VMEM((2, HEADS // 2, 2 * SEQ, SEQ), F32),
            pltpu.VMEM((2, SEQ, 128), F32),
            pltpu.VMEM((2, SEQ, D), BF16),
            pltpu.VMEM((2, SEQ, D), BF16),
            pltpu.VMEM((2, SEQ, 3 * D), BF16),
            pltpu.VMEM((2, SEQ, D), BF16),
            pltpu.VMEM((SEQ, D), BF16),
            pltpu.VMEM((SEQ, D), BF16),
            pltpu.VMEM((16, D), F32),
            pltpu.VMEM((2, 16, SEQ), F32),
            dma((2,)), dma((2,)), dma((2,)), dma((2,)), dma((2,)), dma((2,)),
            dma((2, NX - 1, 4)), dma((2, NX - 1, 4)),
        ],
        compiler_params=pltpu.CompilerParams(
            collective_id=0, has_side_effects=True, vmem_limit_bytes=50 * 2**20
        ),
        name="pipe",
    )(h0, mod, noise, w_qkv, w_out, head)


def reduce_kernel(
    g_ref, out_ref, sq_ref,
    zbuf, ysend, ybuf, tot, sqs, sqz, sqx, sqr,
    z_send, z_recv, y_send, y_recv, x_send, x_recv,
    qz_send, qz_recv, qx_send, qx_recv, qr_send, qr_recv,
):
    s0 = lax.axis_index("section_0")
    s1 = lax.axis_index("section_1")
    d0 = lax.axis_index("dp_0")
    mx = lax.axis_index("dp_1")
    mz = lax.axis_index("dp_2")

    def flip(a, by):
        return 1 - a if by else a

    z_peers = [{"dp_2": lax.rem(mz + d, NZ)} for d in range(1, NZ)]
    x_peers = [{"dp_1": lax.rem(mx + d, NX)} for d in range(1, NX)]
    r_peers = [
        {"section_0": flip(s0, c & 4), "section_1": flip(s1, c & 2), "dp_0": flip(d0, c & 1)}
        for c in range(1, 8)
    ]
    barrier = pltpu.get_barrier_semaphore()
    for where in z_peers + x_peers + r_peers:
        pl.semaphore_signal(barrier, inc=1, device_id=where, device_id_type=MESH)
    pl.semaphore_wait(barrier, 17)

    def remote(src, dst, ssem, rsem, where):
        return pltpu.make_async_remote_copy(
            src_ref=src, dst_ref=dst, send_sem=ssem, recv_sem=rsem,
            device_id=where, device_id_type=MESH,
        )

    z_copies = [
        remote(g_ref.at[:, where["dp_2"]], zbuf.at[i], z_send.at[i], z_recv.at[i], where)
        for i, where in enumerate(z_peers)
    ]
    for copy in z_copies:
        copy.start()
    for copy in z_copies:
        copy.wait_recv()

    def z_sum(i):
        acc = g_ref[i, mz].astype(F32)
        for d in range(NZ - 1):
            acc = acc + zbuf[d, i].astype(F32)
        return acc

    def to_send(i, carry):
        ysend[i] = z_sum((1 - d0) * NX + i)
        return carry

    lax.fori_loop(0, NX, to_send, 0)
    y_copy = remote(ysend, ybuf, y_send.at[0], y_recv.at[0], {"dp_0": 1 - d0})
    y_copy.start()

    def to_keep(i, carry):
        tot[i] = z_sum(d0 * NX + i)
        return carry

    lax.fori_loop(0, NX, to_keep, 0)
    y_copy.wait_recv()

    def add_up(i, acc):
        full = tot[i] + ybuf[i]
        tot[i] = full
        full = full * full
        for c in range(D // 128):
            part = full[:, c * 128 : (c + 1) * 128]
            acc = acc + part[:8] + part[8:]
        return acc

    sqs[0] = lax.fori_loop(0, NX, add_up, jnp.zeros((8, 128), F32))
    x_copies = [
        remote(tot.at[where["dp_1"]], out_ref.at[mx], x_send.at[i], x_recv.at[i], where)
        for i, where in enumerate(x_peers)
    ]

    def sum_over(peers, src, buf, ssem, rsem):
        copies = [
            remote(src, buf.at[i], ssem.at[i], rsem.at[i], where) for i, where in enumerate(peers)
        ]
        for copy in copies:
            copy.start()
        return copies

    def take(copies, src, buf):
        for copy in copies:
            copy.wait_recv()
        acc = src[...]
        for i in range(len(copies)):
            acc = acc + buf[i]
        return acc

    qz = sum_over(z_peers, sqs.at[0], sqz, qz_send, qz_recv)
    for copy in x_copies:
        copy.start()
    out_ref[mx] = tot[mx]
    sqs[1] = take(qz, sqs.at[0], sqz)
    qx = sum_over(x_peers, sqs.at[1], sqx, qx_send, qx_recv)
    sqs[2] = take(qx, sqs.at[1], sqx)
    qr = sum_over(r_peers, sqs.at[2], sqr, qr_send, qr_recv)
    sq_ref[...] = take(qr, sqs.at[2], sqr)
    for copy in x_copies:
        copy.wait_recv()
    for copy in z_copies + [y_copy] + x_copies + qz + qx + qr:
        copy.wait_send()


def run_reduce(grad):
    shape = jax.ShapeDtypeStruct
    dma = pltpu.SemaphoreType.DMA
    return pl.pallas_call(
        reduce_kernel,
        out_shape=(shape((NX, 16, D), F32), shape((8, 128), F32)),
        in_specs=[VMEM],
        out_specs=[VMEM, VMEM],
        scratch_shapes=[
            pltpu.VMEM((NZ - 1, 8, 16, D), BF16),
            pltpu.VMEM((NX, 16, D), F32),
            pltpu.VMEM((NX, 16, D), F32),
            pltpu.VMEM((NX, 16, D), F32),
            pltpu.VMEM((3, 8, 128), F32),
            pltpu.VMEM((NZ - 1, 8, 128), F32),
            pltpu.VMEM((NX - 1, 8, 128), F32),
            pltpu.VMEM((7, 8, 128), F32),
            dma((NZ - 1,)), dma((NZ - 1,)), dma((1,)), dma((1,)), dma((NX - 1,)), dma((NX - 1,)),
            dma((NZ - 1,)), dma((NZ - 1,)), dma((NX - 1,)), dma((NX - 1,)), dma((7,)), dma((7,)),
        ],
        compiler_params=pltpu.CompilerParams(
            collective_id=1, has_side_effects=True, vmem_limit_bytes=32 * 2**20
        ),
        name="reduce",
    )(grad)


def optimizer_step(gradient, moment, second, factor):
    normalized = gradient * factor
    moment_new = 0.9 * moment + 0.1 * normalized
    second_new = 0.99 * second + 0.01 * normalized * normalized
    return (moment_new / (jnp.sqrt(second_new) + 1e-08), moment_new, second_new)


def local(
    latents,
    noise,
    timesteps,
    cameras,
    embed_in,
    camera_table,
    w_mod,
    w_qkv,
    w_out,
    head_out,
    moment_qkv,
    moment_out,
    second_qkv,
    second_out,
):
    time_emb = time_embed(timesteps, w_mod.shape[1])
    modulation = jnp.dot(time_emb, w_mod[0], preferred_element_type=jnp.float32)
    mod = jnp.pad(modulation.reshape(2, 3, D), ((0, 0), (0, 5), (0, 0))).reshape(16, D)
    h0 = jax.vmap(embed_sample, in_axes=(0, 0, 0, 0, None, None))(
        latents, noise, timesteps, cameras, embed_in, camera_table
    )
    noise_rows = jnp.pad(noise.astype(F32), ((0, 0), (0, 12), (0, 0)))
    head = jnp.pad(head_out, ((0, 12), (0, 0)))
    nall, aall, ball, pall = run_pipe(h0, mod, noise_rows, w_qkv[0], w_out[0], head)
    rows = NX * 2 * SEQ
    grad = jnp.concatenate(
        [
            dot_tn(nall.reshape(rows, D), ball.reshape(rows, QB)).astype(BF16),
            dot_tn(aall.reshape(rows, D), pall.reshape(rows, OB)).astype(BF16),
        ],
        axis=1,
    )
    shard, squares = run_reduce(grad.reshape(8, NZ, 16, D))
    factor = lax.rsqrt(jnp.sum(squares) / 16777216.0 + 1e-12)
    qkv_shard = jnp.transpose(shard[:, :, :QB], (1, 0, 2)).reshape(1, 16, 3 * D)
    out_shard = jnp.transpose(shard[:, :, QB:], (1, 0, 2)).reshape(1, 16, D)
    update_qkv, new_moment_qkv, new_second_qkv = optimizer_step(
        qkv_shard, moment_qkv, second_qkv, factor
    )
    update_out, new_moment_out, new_second_out = optimizer_step(
        out_shard, moment_out, second_out, factor
    )
    return (update_qkv, update_out, new_moment_qkv, new_moment_out, new_second_qkv, new_second_out)


def solution(mesh):
    torus = Mesh(
        mesh.devices.reshape(2, 2, 2, 4, 8), ("section_0", "section_1", "dp_0", "dp_1", "dp_2")
    )
    return jax.shard_map(
        local,
        mesh=torus,
        in_specs=(
            P(DP, None, None),
            P(DP, None, None),
            P(DP),
            P(DP, None),
            P(),
            P(),
            P(SECTION, None, None),
            P(SECTION, None, None),
            P(SECTION, None, None),
            P(),
            P(SECTION, DP, None),
            P(SECTION, DP, None),
            P(SECTION, DP, None),
            P(SECTION, DP, None),
        ),
        out_specs=(
            P(SECTION, DP, None),
            P(SECTION, DP, None),
            P(SECTION, DP, None),
            P(SECTION, DP, None),
            P(SECTION, DP, None),
            P(SECTION, DP, None),
        ),
        check_vma=False,
    )
```

```python
import functools
import math

import jax
import jax.numpy as jnp
from jax import lax
from jax.experimental import pallas as pl
from jax.experimental.pallas import tpu as pltpu
from jax.sharding import Mesh
from jax.sharding import PartitionSpec as P

HEADS = 16
HEAD_DIM = 64
SECTION = ("section_0", "section_1")
DP = ("dp_0", "dp_1", "dp_2")
MESH = pl.DeviceIdType.MESH
F32 = jnp.float32
BF16 = jnp.bfloat16
D = 1024
SEQ = 128
NX = 4
NZ = 8
QB = 3 * D // NX
OB = D // NX
VMEM = pl.BlockSpec(memory_space=pltpu.VMEM)
ANY = pl.BlockSpec(memory_space=pl.ANY)


def time_embed(step_ids, emb_width):
    half_dim = emb_width // 2
    frequency = jnp.exp(-math.log(10000.0) * jnp.arange(half_dim, dtype=jnp.float32) / half_dim)
    phases = step_ids.astype(jnp.float32)[:, None] * frequency[None, :]
    joined = jnp.concatenate([jnp.cos(phases), jnp.sin(phases)], axis=-1)
    return jax.nn.silu(joined).astype(jnp.bfloat16)


def embed_sample(latent_now, noise_now, step_now, camera_now, embed_in, camera_table):
    step_f = step_now.astype(jnp.float32)
    alpha_bar = jnp.cos((step_f / 1000.0 + 0.008) / 1.008 * (math.pi / 2.0)) ** 2
    noised = jnp.sqrt(alpha_bar) * latent_now.astype(jnp.float32) + jnp.sqrt(
        1.0 - alpha_bar
    ) * noise_now.astype(jnp.float32)
    features = lax.dot_general(
        noised.astype(jnp.bfloat16),
        embed_in,
        (((0,), (0,)), ((), ())),
        preferred_element_type=jnp.float32,
    )
    onehot = (
        camera_now[:, None] == jnp.arange(camera_table.shape[0], dtype=jnp.int32)[None, :]
    ).astype(jnp.bfloat16)
    camera_vec = jnp.dot(onehot, camera_table, preferred_element_type=jnp.float32)
    model_width = embed_in.shape[1]
    views = camera_now.shape[0]
    joined = features.reshape(views, -1, model_width) + camera_vec[:, None, :]
    return joined.reshape(-1, model_width).astype(jnp.bfloat16)


def dot_nn(a, b):
    return lax.dot_general(a, b, (((1,), (0,)), ((), ())), preferred_element_type=F32)


def dot_nt(a, b):
    return lax.dot_general(a, b, (((1,), (1,)), ((), ())), preferred_element_type=F32)


def dot_tn(a, b):
    return lax.dot_general(a, b, (((0,), (0,)), ((), ())), preferred_element_type=F32)


def lanes(start, size):
    return pl.ds(pl.multiple_of(start, 128), size)


def step_kernel(
    h0_ref, mod_ref, noise_ref, wqkv_hbm, wout_hbm, head_ref,
    outq_ref, outo_ref, factor_ref,
    wqkv_ref, wout_ref, wqkv_t, wout_t, nall, aall, ball, pall, n_t, a_t,
    h_scr, hn_scr, nrm_scr, att_scr, qkv_scr, p_scr, r_scr, g_scr, gs_scr,
    dqkv_scr, pc_scr, datt_scr, tmp_scr, mods, noi,
    up_out, up_in, dn_out, dn_in, summed, y_out, y_in, totq, toto, sqs, sqz, sqx, sqr,
    h_send, h_recv, g_send, g_recv, sw_send, sw_recv, x_send, x_recv,
    up_send, up_recv, dn_send, dn_recv, y_send, y_recv, o_send, o_recv,
    qz_send, qz_recv, qx_send, qx_recv, qr_send, qr_recv, w_sem,
):
    w_copies = [
        pltpu.make_async_copy(wqkv_hbm, wqkv_ref, w_sem.at[0]),
        pltpu.make_async_copy(wout_hbm, wout_ref, w_sem.at[1]),
    ]
    for copy in w_copies:
        copy.start()
    s0 = lax.axis_index("section_0")
    s1 = lax.axis_index("section_1")
    d0 = lax.axis_index("dp_0")
    mx = lax.axis_index("dp_1")
    mz = lax.axis_index("dp_2")
    sec = 2 * s0 + s1

    def toward(step):
        other = sec + step
        o0 = lax.rem(lax.div(other + 4, 2), 2)
        o1 = lax.rem(other + 4, 2)
        crossing = (o0 + s0) - 2 * o0 * s0
        od = (d0 + crossing) - 2 * d0 * crossing
        return {"section_0": o0, "section_1": o1, "dp_0": od}

    nxt = toward(1)
    prv = toward(-1)
    partner = {"dp_0": 1 - d0}

    barrier = pltpu.get_barrier_semaphore()

    def greet(where):
        pl.semaphore_signal(barrier, inc=1, device_id=where, device_id_type=MESH)

    def flip(a, by):
        return 1 - a if by else a

    z_peers = [{"dp_2": lax.rem(mz + d, NZ)} for d in range(1, NZ)]
    x_peers = [{"dp_1": lax.rem(mx + d, NX)} for d in range(1, NX)]
    r_peers = [
        {"section_0": flip(s0, c & 4), "section_1": flip(s1, c & 2), "dp_0": flip(d0, c & 1)}
        for c in range(1, 8)
    ]
    for where in z_peers + x_peers + r_peers:
        greet(where)

    @pl.when(sec < 3)
    def _():
        greet(nxt)

    @pl.when(sec > 0)
    def _():
        greet(prv)

    pl.semaphore_wait(barrier, 17 + lax.min(sec, 1) + lax.min(3 - sec, 1))

    def remote(src, dst, ssem, rsem, where):
        return pltpu.make_async_remote_copy(
            src_ref=src, dst_ref=dst, send_sem=ssem, recv_sem=rsem,
            device_id=where, device_id_type=MESH,
        )

    def swap_mod():
        return remote(mod_ref, mods, sw_send.at[0], sw_recv.at[0], partner)

    def swap_noise():
        return remote(noise_ref, noi, sw_send.at[1], sw_recv.at[1], partner)

    @pl.when(s0 == 1)
    def _():
        swap_mod().start()
        swap_noise().start()
        swap_mod().wait_recv()
        swap_noise().wait_recv()

    @pl.when(s0 == 0)
    def _():
        mods[...] = mod_ref[...]

    def h_copy(m, n):
        cols = pl.ds(n * 512, 512)
        return remote(
            hn_scr.at[m, :, cols], h_scr.at[m, :, cols], h_send.at[m, n], h_recv.at[m, n], nxt
        )

    def g_copy(m):
        return remote(gs_scr.at[m], g_scr.at[m], g_send.at[m], g_recv.at[m], prv)

    def rows_of(src, m):
        return pl.ds(pl.multiple_of(src * 2 * SEQ + m * SEQ, SEQ), SEQ)

    def x_copy(m, d, k):
        to = lax.rem(mx + d, NX)
        rows = rows_of(mx, m)
        src, dst = (
            (nrm_scr.at[m], nall.at[rows]),
            (att_scr.at[m], aall.at[rows]),
            (pc_scr.at[m, :, lanes(to * OB, OB)], pall.at[rows]),
        )[k] if k < 3 else (
            dqkv_scr.at[m, :, lanes(to * QB + (k - 3) * OB, OB)],
            ball.at[rows, pl.ds((k - 3) * OB, OB)],
        )
        return remote(src, dst, x_send.at[m, d - 1, k], x_recv.at[m, d - 1, k], {"dp_1": to})

    def act_copies(m):
        return [x_copy(m, d, k) for k in (0, 1) for d in (1, 3)]

    def cot_copies(m, k):
        return [x_copy(m, d, k) for d in (1, 2, 3)]

    def relays(m):
        left, right = lax.rem(mx + 3, NX), lax.rem(mx + 1, NX)
        nrows, arows = rows_of(left, m), rows_of(right, m)
        return [
            remote(
                nall.at[nrows], nall.at[nrows], x_send.at[m, 1, 0], x_recv.at[m, 1, 0],
                {"dp_1": right},
            ),
            remote(
                aall.at[arows], aall.at[arows], x_send.at[m, 1, 1], x_recv.at[m, 1, 1],
                {"dp_1": left},
            ),
        ]

    def relay(m):
        x_copy(m, 1, 0).wait_recv()
        x_copy(m, 3, 1).wait_recv()
        for copy in relays(m):
            copy.start()

    low = lax.broadcasted_iota(jnp.int32, (SEQ, 128), 1) < HEAD_DIM

    def both(tile):
        zero = jnp.zeros_like(tile)
        return jnp.concatenate([jnp.where(low, tile, zero), jnp.where(low, zero, tile)], axis=0)

    def merged(pair):
        return jnp.where(low, pair[:SEQ], pair[SEQ:])

    PAIRS = HEADS // 2
    GROUP = 4

    def over_pairs(body):
        def step(i, carry):
            for j in range(GROUP):
                body(i * GROUP + j)
            return carry

        lax.fori_loop(0, PAIRS // GROUP, step, 0)

    def forward(m, carry):
        @pl.when(sec == 0)
        def _():
            h_scr[m] = h0_ref[m]

        @pl.when(sec > 0)
        def _():
            h_copy(m, 0).wait_recv()
            h_copy(m, 1).wait_recv()

        shift = mods[pl.ds(m, 1), pl.ds(0, D)]
        scale = mods[pl.ds(m, 1), pl.ds(D, D)]
        gate = mods[pl.ds(m, 1), pl.ds(2 * D, D)]
        hf = h_scr[m].astype(F32)
        r = lax.rsqrt(jnp.mean(hf * hf, axis=-1, keepdims=True) + 1e-06)
        r_scr[m] = jnp.broadcast_to(r, (SEQ, 128))
        nrm_scr[m] = (hf * r * (1.0 + scale) + shift).astype(BF16)
        for n in range(6):
            cols = pl.ds(n * 512, 512)
            qkv_scr[m, :, cols] = dot_nn(nrm_scr[m], wqkv_ref[:, cols]).astype(BF16)

        def pair(j):
            q = qkv_scr[m, :, lanes(j * 128, 128)]
            k = qkv_scr[m, :, lanes(D + j * 128, 128)]
            v = qkv_scr[m, :, lanes(2 * D + j * 128, 128)]
            s = dot_nt(both(q), k) * (1.0 / math.sqrt(HEAD_DIM))
            s = jnp.exp(s - jnp.max(s, axis=-1, keepdims=True))
            p = s / jnp.sum(s, axis=-1, keepdims=True)
            p_scr[m, j] = p
            att_scr[m, :, lanes(j * 128, 128)] = merged(dot_nn(p.astype(BF16), v)).astype(BF16)

        over_pairs(pair)
        for n in range(2):
            cols = pl.ds(n * 512, 512)
            proj = dot_nn(att_scr[m], wout_ref[:, cols])
            hn_scr[m, :, cols] = (
                h_scr[m, :, cols].astype(F32) + gate[:, n * 512 : (n + 1) * 512] * proj
            ).astype(BF16)

            @pl.when(sec < 3)
            def _():
                h_copy(m, n).start()

        for copy in act_copies(m):
            copy.start()
        rows = rows_of(mx, m)
        nall[rows] = nrm_scr[m]
        aall[rows] = att_scr[m]

        @pl.when(sec == 3)
        def _():
            ff = hn_scr[m].astype(F32)
            rr = lax.rsqrt(jnp.mean(ff * ff, axis=-1, keepdims=True) + 1e-06)
            predicted = dot_nt(head_ref[...], (ff * rr).astype(BF16))
            err = 2.0 * (predicted - noi[m])
            hi = err.astype(BF16)
            lo = (err - hi.astype(F32)).astype(BF16)
            dn = (dot_tn(hi, head_ref[...]) + dot_tn(lo, head_ref[...])).astype(BF16).astype(F32)
            inner = jnp.sum(dn * ff, axis=-1, keepdims=True) * (1.0 / D)
            g_scr[m] = (dn * rr - ff * (rr * rr * rr * inner)).astype(BF16)

        return carry

    def turn_weights():
        def block(i, carry):
            here = lanes(i * 128, 128)
            for src, dst, tiles in ((wqkv_ref, wqkv_t, 24), (wout_ref, wout_t, 8)):
                for g in range(tiles):
                    dst[pl.ds(g * 128, 128), here] = jnp.transpose(src[here, pl.ds(g * 128, 128)])
            return carry

        lax.fori_loop(0, 8, block, 0)

    for copy in w_copies:
        copy.wait()

    @pl.when(s0 == 1)
    def _():
        turn_weights()

    lax.fori_loop(0, 2, forward, 0)

    def turn():
        def arrived(m, carry):
            x_copy(m, 3, 0).wait_recv()
            x_copy(m, 1, 1).wait_recv()
            for copy in relays(m):
                copy.wait_recv()
            return carry

        lax.fori_loop(0, 2, arrived, 0)

        def block(i, carry):
            here = lanes(i * SEQ, SEQ)
            for src, dst in ((nall, n_t), (aall, a_t)):
                for g in range(8):
                    tile = src[here, pl.ds(g * 128, 128)]
                    dst[g, :, :, here] = jnp.transpose(tile).reshape(NZ, 16, SEQ)
            return carry

        lax.fori_loop(0, 2 * NX, block, 0)

    @pl.when(sec < 3)
    def _():
        relay(0)

    @pl.when(s0 == 0)
    def _():
        relay(1)
        turn_weights()
        turn()

    def backward(m, carry):
        @pl.when(sec < 3)
        def _():
            g_copy(m).wait_recv()

        scale = mods[pl.ds(m, 1), pl.ds(D, D)]
        gate = mods[pl.ds(m, 1), pl.ds(2 * D, D)]
        pc_scr[m] = (gate * g_scr[m].astype(F32)).astype(BF16)
        for copy in cot_copies(m, 2):
            copy.start()
        for n in range(2):
            cols = pl.ds(n * 512, 512)
            datt_scr[:, cols] = dot_nn(pc_scr[m], wout_t[:, cols]).astype(BF16)

        def pair(j):
            cq, ck, cv = lanes(j * 128, 128), lanes(D + j * 128, 128), lanes(2 * D + j * 128, 128)
            q2 = both(qkv_scr[m, :, cq])
            k = qkv_scr[m, :, ck]
            v = qkv_scr[m, :, cv]
            do2 = both(datt_scr[:, cq])
            p = p_scr[m, j]
            dv = dot_tn(p.astype(BF16), do2)
            dp = dot_nt(do2, v).astype(BF16).astype(F32)
            ds = p * (dp - jnp.sum(dp * p, axis=-1, keepdims=True))
            ds = (ds * (1.0 / math.sqrt(HEAD_DIM))).astype(BF16)
            dqkv_scr[m, :, cv] = dv.astype(BF16)
            dqkv_scr[m, :, cq] = merged(dot_nn(ds, k)).astype(BF16)
            dqkv_scr[m, :, ck] = dot_tn(ds, q2).astype(BF16)

        over_pairs(pair)
        for k in (3, 4, 5):
            for copy in cot_copies(m, k):
                copy.start()

        @pl.when(sec > 0)
        def _():
            for n in range(2):
                cols = pl.ds(n * 512, 512)
                tmp_scr[:, cols] = dot_nn(dqkv_scr[m], wqkv_t[:, cols]).astype(BF16)
            hf = h_scr[m].astype(F32)
            r = r_scr[m][:, :1]
            u = tmp_scr[...].astype(F32) * (1.0 + scale)
            inner = jnp.sum(u * hf, axis=-1, keepdims=True) * (1.0 / D)
            dh = (u * r - hf * (r * r * r * inner)).astype(BF16).astype(F32)
            gs_scr[m] = (dh + g_scr[m].astype(F32)).astype(BF16)
            g_copy(m).start()

        rows = rows_of(mx, m)
        ball[rows] = dqkv_scr[m, :, lanes(mx * QB, QB)]
        pall[rows] = pc_scr[m, :, lanes(mx * OB, OB)]

        @pl.when((sec == 2) & (m == 0))
        def _():
            relay(1)

        return carry

    lax.fori_loop(0, 2, backward, 0)

    @pl.when(sec == 3)
    def _():
        relay(0)
        relay(1)

    @pl.when(s0 == 1)
    def _():
        turn()

    def exchanged(quarter):
        def arrive(m, carry):
            for copy in cot_copies(m, 2 + quarter):
                copy.wait_recv()
            return carry

        lax.fori_loop(0, 2, arrive, 0)

    def partial(dest, quarter):
        left = (n_t if quarter else a_t)[:, dest].reshape(8 * 16, NX * 2 * SEQ)
        if quarter == 0:
            return dot_nn(left, pall[...])
        return dot_nn(left, ball[:, pl.ds((quarter - 1) * OB, OB)])

    z_up = {"dp_2": lax.rem(mz + 1, NZ)}
    z_dn = {"dp_2": lax.rem(mz + NZ - 1, NZ)}

    def ring_copy(up, t, quarter):
        k = 4 * quarter + t
        if up:
            return remote(up_out.at[k], up_in.at[k], up_send.at[k], up_recv.at[k], z_up)
        return remote(dn_out.at[k], dn_in.at[k], dn_send.at[k], dn_recv.at[k], z_dn)

    def hops(up, quarter):
        return 4 if up == (quarter % 2 == 0) else 3

    def y_copy(quarter):
        return remote(
            y_out.at[quarter], y_in.at[quarter], y_send.at[quarter], y_recv.at[quarter], partner
        )

    def ring_step(up, t, quarter):
        n = hops(up, quarter)
        if t >= n:
            return
        out, got = (up_out, up_in) if up else (dn_out, dn_in)
        val = partial(lax.rem(mz + NZ + (n - t if up else t - n), NZ), quarter)
        if t > 0:
            ring_copy(up, t - 1, quarter).wait_recv()
            val = val + got[4 * quarter + t - 1].astype(F32)
        out[4 * quarter + t] = val.astype(BF16)
        ring_copy(up, t, quarter).start()

    def ring_end(quarter):
        val = partial(mz, quarter)
        for up in (True, False):
            n = hops(up, quarter)
            ring_copy(up, n - 1, quarter).wait_recv()
            val = val + (up_in if up else dn_in)[4 * quarter + n - 1].astype(F32)
        summed[quarter] = val.reshape(2, NX * 16, OB)
        y_out[quarter] = summed[quarter, 1 - d0].astype(BF16)
        y_copy(quarter).start()

    def o_copies(quarter):
        made = []
        for i, where in enumerate(x_peers):
            if quarter == 0:
                src, dst = toto.at[where["dp_1"]], outo_ref.at[:, lanes(mx * OB, OB)]
            else:
                src = totq.at[quarter - 1, where["dp_1"]]
                dst = outq_ref.at[:, lanes(mx * QB + (quarter - 1) * OB, OB)]
            made.append(remote(src, dst, o_send.at[quarter, i], o_recv.at[quarter, i], where))
        return made

    def y_end(quarter, acc):
        y_copy(quarter).wait_recv()
        full = summed[quarter, d0] + y_in[quarter].astype(F32)
        by_x = full.reshape(NX, 16, OB)
        if quarter == 0:
            toto[...] = by_x
        else:
            totq[quarter - 1] = by_x
        for copy in o_copies(quarter):
            copy.start()
        full = full * full
        for c in range(2):
            for i in range(NX * 2):
                acc = acc + full[i * 8 : (i + 1) * 8, c * 128 : (c + 1) * 128]
        return acc

    acc = jnp.zeros((8, 128), F32)
    for wave in range(9):
        for quarter in range(4):
            t = wave - quarter
            if t == 0:
                exchanged(quarter)
            if 0 <= t < 4:
                for up in (True, False):
                    ring_step(up, t, quarter)
            if t == 4:
                ring_end(quarter)
            if t == 5:
                acc = y_end(quarter, acc)
    sqs[0] = acc

    def sum_over(peers, src, buf, ssem, rsem):
        copies = [
            remote(src, buf.at[i], ssem.at[i], rsem.at[i], where) for i, where in enumerate(peers)
        ]
        for copy in copies:
            copy.start()
        return copies

    def take(copies, src, buf):
        for copy in copies:
            copy.wait_recv()
        acc = src[...]
        for i in range(len(copies)):
            acc = acc + buf[i]
        return acc

    qz = sum_over(z_peers, sqs.at[0], sqz, qz_send, qz_recv)
    outo_ref[:, lanes(mx * OB, OB)] = toto[mx]
    for quarter in range(1, 4):
        outq_ref[:, lanes(mx * QB + (quarter - 1) * OB, OB)] = totq[quarter - 1, mx]
    sqs[1] = take(qz, sqs.at[0], sqz)
    qx = sum_over(x_peers, sqs.at[1], sqx, qx_send, qx_recv)
    sqs[2] = take(qx, sqs.at[1], sqx)
    qr = sum_over(r_peers, sqs.at[2], sqr, qr_send, qr_recv)
    total = take(qr, sqs.at[2], sqr)
    total = jnp.sum(jnp.sum(total, axis=1, keepdims=True), axis=0, keepdims=True)
    factor_ref[...] = jnp.broadcast_to(lax.rsqrt(total / 16777216.0 + 1e-12), (8, 128))
    for quarter in range(4):
        for copy in o_copies(quarter):
            copy.wait_recv()
    for quarter in range(4):
        for up in (True, False):
            for t in range(hops(up, quarter)):
                ring_copy(up, t, quarter).wait_send()
        y_copy(quarter).wait_send()
        for copy in o_copies(quarter):
            copy.wait_send()
    for copy in qz + qx + qr:
        copy.wait_send()

    def finish(m, carry):
        for copy in act_copies(m) + relays(m):
            copy.wait_send()
        for k in (2, 3, 4, 5):
            for copy in cot_copies(m, k):
                copy.wait_send()

        @pl.when(sec < 3)
        def _():
            h_copy(m, 0).wait_send()
            h_copy(m, 1).wait_send()

        @pl.when(sec > 0)
        def _():
            g_copy(m).wait_send()

        return carry

    lax.fori_loop(0, 2, finish, 0)

    @pl.when(s0 == 1)
    def _():
        swap_mod().wait_send()
        swap_noise().wait_send()


def run_step(h0, mod, noise, w_qkv, w_out, head):
    shape = jax.ShapeDtypeStruct
    dma = pltpu.SemaphoreType.DMA
    vmem = pltpu.VMEM
    rows = NX * 2 * SEQ
    return pl.pallas_call(
        step_kernel,
        out_shape=(shape((16, 3 * D), F32), shape((16, D), F32), shape((8, 128), F32)),
        in_specs=[VMEM, VMEM, VMEM, ANY, ANY, VMEM],
        out_specs=[VMEM] * 3,
        scratch_shapes=[
            vmem((D, 3 * D), BF16),
            vmem((D, D), BF16),
            vmem((3 * D, D), BF16),
            vmem((D, D), BF16),
            vmem((rows, D), BF16),
            vmem((rows, D), BF16),
            vmem((rows, QB), BF16),
            vmem((rows, OB), BF16),
            vmem((8, NZ, 16, rows), BF16),
            vmem((8, NZ, 16, rows), BF16),
            vmem((2, SEQ, D), BF16),
            vmem((2, SEQ, D), BF16),
            vmem((2, SEQ, D), BF16),
            vmem((2, SEQ, D), BF16),
            vmem((2, SEQ, 3 * D), BF16),
            vmem((2, HEADS // 2, 2 * SEQ, SEQ), F32),
            vmem((2, SEQ, 128), F32),
            vmem((2, SEQ, D), BF16),
            vmem((2, SEQ, D), BF16),
            vmem((2, SEQ, 3 * D), BF16),
            vmem((2, SEQ, D), BF16),
            vmem((SEQ, D), BF16),
            vmem((SEQ, D), BF16),
            vmem((8, 3 * D), F32),
            vmem((2, 16, SEQ), F32),
            vmem((16, 128, OB), BF16),
            vmem((16, 128, OB), BF16),
            vmem((16, 128, OB), BF16),
            vmem((16, 128, OB), BF16),
            vmem((4, 2, NX * 16, OB), F32),
            vmem((4, NX * 16, OB), BF16),
            vmem((4, NX * 16, OB), BF16),
            vmem((3, NX, 16, OB), F32),
            vmem((NX, 16, OB), F32),
            vmem((3, 8, 128), F32),
            vmem((NZ - 1, 8, 128), F32),
            vmem((NX - 1, 8, 128), F32),
            vmem((7, 8, 128), F32),
            dma((2, 2)), dma((2, 2)), dma((2,)), dma((2,)), dma((2,)), dma((2,)),
            dma((2, NX - 1, 6)), dma((2, NX - 1, 6)),
            dma((16,)), dma((16,)), dma((16,)), dma((16,)), dma((4,)), dma((4,)),
            dma((4, NX - 1)), dma((4, NX - 1)),
            dma((NZ - 1,)), dma((NZ - 1,)), dma((NX - 1,)), dma((NX - 1,)), dma((7,)), dma((7,)),
            dma((2,)),
        ],
        compiler_params=pltpu.CompilerParams(
            collective_id=0, has_side_effects=True, vmem_limit_bytes=58 * 2**20
        ),
        name="step",
    )(h0, mod, noise, w_qkv, w_out, head)


def optimizer_kernel(gq, go, factor_ref, mq, mo, vq, vo, uq, uo, nmq, nmo, nvq, nvo):
    factor = factor_ref[0:1, 0:1]
    for g, m, v, u, nm, nv in ((gq, mq, vq, uq, nmq, nvq), (go, mo, vo, uo, nmo, nvo)):
        normalized = g[...] * factor
        moment = 0.9 * m[0] + 0.1 * normalized
        second = 0.99 * v[0] + 0.01 * normalized * normalized
        u[0] = moment / (jnp.sqrt(second) + 1e-08)
        nm[0] = moment
        nv[0] = second


def optimizer(gq, go, factor, mq, mo, vq, vo):
    shape = jax.ShapeDtypeStruct
    big, small = shape((1, 16, 3 * D), F32), shape((1, 16, D), F32)
    return pl.pallas_call(
        optimizer_kernel,
        out_shape=(big, small, big, small, big, small),
        in_specs=[VMEM] * 7,
        out_specs=[VMEM] * 6,
        name="optimizer",
    )(gq, go, factor, mq, mo, vq, vo)


def local(
    latents,
    noise,
    timesteps,
    cameras,
    embed_in,
    camera_table,
    w_mod,
    w_qkv,
    w_out,
    head_out,
    moment_qkv,
    moment_out,
    second_qkv,
    second_out,
):
    time_emb = time_embed(timesteps, w_mod.shape[1])
    time_rows = jnp.pad(time_emb, ((0, 6), (0, 0)))
    mod = jnp.dot(time_rows, w_mod[0], preferred_element_type=jnp.float32)
    h0 = jax.vmap(embed_sample, in_axes=(0, 0, 0, 0, None, None))(
        latents, noise, timesteps, cameras, embed_in, camera_table
    )
    noise_rows = jnp.pad(noise.astype(F32), ((0, 0), (0, 12), (0, 0)))
    head = jnp.pad(head_out, ((0, 12), (0, 0)))
    qkv_rows, out_rows, factors = run_step(h0, mod, noise_rows, w_qkv[0], w_out[0], head)
    return optimizer(
        qkv_rows, out_rows, factors, moment_qkv, moment_out, second_qkv, second_out
    )


def solution(mesh):
    torus = Mesh(
        mesh.devices.reshape(2, 2, 2, 4, 8), ("section_0", "section_1", "dp_0", "dp_1", "dp_2")
    )
    return jax.shard_map(
        local,
        mesh=torus,
        in_specs=(
            P(DP, None, None),
            P(DP, None, None),
            P(DP),
            P(DP, None),
            P(),
            P(),
            P(SECTION, None, None),
            P(SECTION, None, None),
            P(SECTION, None, None),
            P(),
            P(SECTION, DP, None),
            P(SECTION, DP, None),
            P(SECTION, DP, None),
            P(SECTION, DP, None),
        ),
        out_specs=(
            P(SECTION, DP, None),
            P(SECTION, DP, None),
            P(SECTION, DP, None),
            P(SECTION, DP, None),
            P(SECTION, DP, None),
            P(SECTION, DP, None),
        ),
        check_vma=False,
    )
```

```python
import functools
import math

import jax
import jax.numpy as jnp
from jax import lax
from jax.experimental import pallas as pl
from jax.experimental.pallas import tpu as pltpu
from jax.sharding import Mesh
from jax.sharding import PartitionSpec as P

HEADS = 16
HEAD_DIM = 64
SECTION = ("section_0", "section_1")
DP = ("dp_0", "dp_1", "dp_2")
MESH = pl.DeviceIdType.MESH
F32 = jnp.float32
BF16 = jnp.bfloat16
D = 1024
SEQ = 128
NX = 4
NZ = 8
QB = 3 * D // NX
OB = D // NX
VMEM = pl.BlockSpec(memory_space=pltpu.VMEM)
ANY = pl.BlockSpec(memory_space=pl.ANY)


def time_embed(step_ids, emb_width):
    half_dim = emb_width // 2
    frequency = jnp.exp(-math.log(10000.0) * jnp.arange(half_dim, dtype=jnp.float32) / half_dim)
    phases = step_ids.astype(jnp.float32)[:, None] * frequency[None, :]
    joined = jnp.concatenate([jnp.cos(phases), jnp.sin(phases)], axis=-1)
    return jax.nn.silu(joined).astype(jnp.bfloat16)


def embed_sample(latent_now, noise_now, step_now, camera_now, embed_in, camera_table):
    step_f = step_now.astype(jnp.float32)
    alpha_bar = jnp.cos((step_f / 1000.0 + 0.008) / 1.008 * (math.pi / 2.0)) ** 2
    noised = jnp.sqrt(alpha_bar) * latent_now.astype(jnp.float32) + jnp.sqrt(
        1.0 - alpha_bar
    ) * noise_now.astype(jnp.float32)
    features = lax.dot_general(
        noised.astype(jnp.bfloat16),
        embed_in,
        (((0,), (0,)), ((), ())),
        preferred_element_type=jnp.float32,
    )
    onehot = (
        camera_now[:, None] == jnp.arange(camera_table.shape[0], dtype=jnp.int32)[None, :]
    ).astype(jnp.bfloat16)
    camera_vec = jnp.dot(onehot, camera_table, preferred_element_type=jnp.float32)
    model_width = embed_in.shape[1]
    views = camera_now.shape[0]
    joined = features.reshape(views, -1, model_width) + camera_vec[:, None, :]
    return joined.reshape(-1, model_width).astype(jnp.bfloat16)


def dot_nn(a, b):
    return lax.dot_general(a, b, (((1,), (0,)), ((), ())), preferred_element_type=F32)


def dot_nt(a, b):
    return lax.dot_general(a, b, (((1,), (1,)), ((), ())), preferred_element_type=F32)


def dot_tn(a, b):
    return lax.dot_general(a, b, (((0,), (0,)), ((), ())), preferred_element_type=F32)


def lanes(start, size):
    return pl.ds(pl.multiple_of(start, 128), size)


def step_kernel(
    h0_ref, mod_ref, noise_ref, wqkv_hbm, wout_hbm, head_ref,
    outq_ref, outo_ref, factor_ref,
    wqkv_ref, wout_ref, wqkv_t, wout_t, nall, aall, ball, pall, n_t, a_t,
    h_scr, hn_scr, nrm_scr, att_scr, qkv_scr, p_scr, r_scr, g_scr, gs_scr,
    dqkv_scr, pc_scr, datt_scr, tmp_scr, mods, noi,
    up_out, up_in, dn_out, dn_in, c_sum, c_out, c_in, summed, y_out, y_in, totq, toto, sqs, sqz, sqx, sqr,
    h_send, h_recv, g_send, g_recv, sw_send, sw_recv, x_send, x_recv,
    up_send, up_recv, dn_send, dn_recv, c_send, c_recv, y_send, y_recv, o_send, o_recv,
    qz_send, qz_recv, qx_send, qx_recv, qr_send, qr_recv, w_sem,
):
    w_copies = [
        pltpu.make_async_copy(wqkv_hbm, wqkv_ref, w_sem.at[0]),
        pltpu.make_async_copy(wout_hbm, wout_ref, w_sem.at[1]),
    ]
    for copy in w_copies:
        copy.start()
    s0 = lax.axis_index("section_0")
    s1 = lax.axis_index("section_1")
    d0 = lax.axis_index("dp_0")
    mx = lax.axis_index("dp_1")
    mz = lax.axis_index("dp_2")
    sec = 2 * s0 + s1

    def toward(step):
        other = sec + step
        o0 = lax.rem(lax.div(other + 4, 2), 2)
        o1 = lax.rem(other + 4, 2)
        crossing = (o0 + s0) - 2 * o0 * s0
        od = (d0 + crossing) - 2 * d0 * crossing
        return {"section_0": o0, "section_1": o1, "dp_0": od}

    nxt = toward(1)
    prv = toward(-1)
    partner = {"dp_0": 1 - d0}

    barrier = pltpu.get_barrier_semaphore()

    def greet(where):
        pl.semaphore_signal(barrier, inc=1, device_id=where, device_id_type=MESH)

    def flip(a, by):
        return 1 - a if by else a

    z_peers = [{"dp_2": lax.rem(mz + d, NZ)} for d in range(1, NZ)]
    x_peers = [{"dp_1": lax.rem(mx + d, NX)} for d in range(1, NX)]
    r_peers = [
        {"section_0": flip(s0, c & 4), "section_1": flip(s1, c & 2), "dp_0": flip(d0, c & 1)}
        for c in range(1, 8)
    ]
    for where in z_peers + x_peers + r_peers:
        greet(where)

    @pl.when(sec < 3)
    def _():
        greet(nxt)

    @pl.when(sec > 0)
    def _():
        greet(prv)

    pl.semaphore_wait(barrier, 17 + lax.min(sec, 1) + lax.min(3 - sec, 1))

    def remote(src, dst, ssem, rsem, where):
        return pltpu.make_async_remote_copy(
            src_ref=src, dst_ref=dst, send_sem=ssem, recv_sem=rsem,
            device_id=where, device_id_type=MESH,
        )

    def swap_mod():
        return remote(mod_ref, mods, sw_send.at[0], sw_recv.at[0], partner)

    def swap_noise():
        return remote(noise_ref, noi, sw_send.at[1], sw_recv.at[1], partner)

    @pl.when(s0 == 1)
    def _():
        swap_mod().start()
        swap_noise().start()
        swap_mod().wait_recv()
        swap_noise().wait_recv()

    @pl.when(s0 == 0)
    def _():
        mods[...] = mod_ref[...]

    def h_copy(m, n):
        cols = pl.ds(n * 512, 512)
        return remote(
            hn_scr.at[m, :, cols], h_scr.at[m, :, cols], h_send.at[m, n], h_recv.at[m, n], nxt
        )

    def g_copy(m):
        return remote(gs_scr.at[m], g_scr.at[m], g_send.at[m], g_recv.at[m], prv)

    def rows_of(src, m):
        return pl.ds(pl.multiple_of(src * 2 * SEQ + m * SEQ, SEQ), SEQ)

    def x_copy(m, d, k):
        to = lax.rem(mx + d, NX)
        rows = rows_of(mx, m)
        src, dst = (
            (nrm_scr.at[m], nall.at[rows]),
            (att_scr.at[m], aall.at[rows]),
            (pc_scr.at[m, :, lanes(to * OB, OB)], pall.at[rows]),
        )[k] if k < 3 else (
            dqkv_scr.at[m, :, lanes(to * QB + (k - 3) * OB, OB)],
            ball.at[rows, pl.ds((k - 3) * OB, OB)],
        )
        return remote(src, dst, x_send.at[m, d - 1, k], x_recv.at[m, d - 1, k], {"dp_1": to})

    def act_copies(m, k):
        return [x_copy(m, d, k) for d in (1, 3)]

    def cot_copies(m, k):
        return [x_copy(m, d, k) for d in (1, 2, 3)]

    def relay_copy(m, k):
        by = 1 if k == 0 else 3
        rows = rows_of(lax.rem(mx + NX - by, NX), m)
        held = (nall, aall)[k].at[rows]
        return remote(
            held, held, x_send.at[m, 1, k], x_recv.at[m, 1, k], {"dp_1": lax.rem(mx + by, NX)}
        )

    def relay(m, k):
        x_copy(m, 1 if k == 0 else 3, k).wait_recv()
        relay_copy(m, k).start()

    low = lax.broadcasted_iota(jnp.int32, (SEQ, 128), 1) < HEAD_DIM

    def both(tile):
        zero = jnp.zeros_like(tile)
        return jnp.concatenate([jnp.where(low, tile, zero), jnp.where(low, zero, tile)], axis=0)

    def merged(pair):
        return jnp.where(low, pair[:SEQ], pair[SEQ:])

    PAIRS = HEADS // 2
    GROUP = 4

    def over_pairs(body):
        def step(i, carry):
            for j in range(GROUP):
                body(i * GROUP + j)
            return carry

        lax.fori_loop(0, PAIRS // GROUP, step, 0)

    def forward(m, carry):
        @pl.when(sec == 0)
        def _():
            h_scr[m] = h0_ref[m]

        @pl.when(sec > 0)
        def _():
            h_copy(m, 0).wait_recv()
            h_copy(m, 1).wait_recv()

        shift = mods[pl.ds(m, 1), pl.ds(0, D)]
        scale = mods[pl.ds(m, 1), pl.ds(D, D)]
        gate = mods[pl.ds(m, 1), pl.ds(2 * D, D)]
        hf = h_scr[m].astype(F32)
        r = lax.rsqrt(jnp.mean(hf * hf, axis=-1, keepdims=True) + 1e-06)
        r_scr[m] = jnp.broadcast_to(r, (SEQ, 128))
        nrm_scr[m] = (hf * r * (1.0 + scale) + shift).astype(BF16)
        for n in range(6):
            cols = pl.ds(n * 512, 512)
            qkv_scr[m, :, cols] = dot_nn(nrm_scr[m], wqkv_ref[:, cols]).astype(BF16)

        def pair(j):
            q = qkv_scr[m, :, lanes(j * 128, 128)]
            k = qkv_scr[m, :, lanes(D + j * 128, 128)]
            v = qkv_scr[m, :, lanes(2 * D + j * 128, 128)]
            s = dot_nt(both(q), k) * (1.0 / math.sqrt(HEAD_DIM))
            s = jnp.exp(s - jnp.max(s, axis=-1, keepdims=True))
            p = s / jnp.sum(s, axis=-1, keepdims=True)
            p_scr[m, j] = p
            att_scr[m, :, lanes(j * 128, 128)] = merged(dot_nn(p.astype(BF16), v)).astype(BF16)

        over_pairs(pair)
        for n in range(2):
            cols = pl.ds(n * 512, 512)
            proj = dot_nn(att_scr[m], wout_ref[:, cols])
            hn_scr[m, :, cols] = (
                h_scr[m, :, cols].astype(F32) + gate[:, n * 512 : (n + 1) * 512] * proj
            ).astype(BF16)

            @pl.when(sec < 3)
            def _():
                h_copy(m, n).start()

        for copy in act_copies(m, 0):
            copy.start()
        rows = rows_of(mx, m)
        nall[rows] = nrm_scr[m]

        @pl.when(s0 == 0)
        def _():
            for copy in act_copies(m, 1):
                copy.start()
            aall[rows] = att_scr[m]

        @pl.when(sec == 3)
        def _():
            ff = hn_scr[m].astype(F32)
            rr = lax.rsqrt(jnp.mean(ff * ff, axis=-1, keepdims=True) + 1e-06)
            predicted = dot_nt(head_ref[...], (ff * rr).astype(BF16))
            err = 2.0 * (predicted - noi[m])
            hi = err.astype(BF16)
            lo = (err - hi.astype(F32)).astype(BF16)
            dn = (dot_tn(hi, head_ref[...]) + dot_tn(lo, head_ref[...])).astype(BF16).astype(F32)
            inner = jnp.sum(dn * ff, axis=-1, keepdims=True) * (1.0 / D)
            g_scr[m] = (dn * rr - ff * (rr * rr * rr * inner)).astype(BF16)

        return carry

    def turn_weights():
        def block(i, carry):
            here = lanes(i * 128, 128)
            for src, dst, tiles in ((wqkv_ref, wqkv_t, 24), (wout_ref, wout_t, 8)):
                for g in range(tiles):
                    dst[pl.ds(g * 128, 128), here] = jnp.transpose(src[here, pl.ds(g * 128, 128)])
            return carry

        lax.fori_loop(0, 8, block, 0)

    for copy in w_copies:
        copy.wait()

    @pl.when(s0 == 1)
    def _():
        turn_weights()

    lax.fori_loop(0, 2, forward, 0)

    def turn(k):
        def arrived(m, carry):
            x_copy(m, 3 if k == 0 else 1, k).wait_recv()
            relay_copy(m, k).wait_recv()
            return carry

        lax.fori_loop(0, 2, arrived, 0)

        def block(i, carry):
            here = lanes(i * SEQ, SEQ)
            src, dst = ((nall, n_t), (aall, a_t))[k]
            for g in range(8):
                tile = src[here, pl.ds(g * 128, 128)]
                dst[g, :, :, here] = jnp.transpose(tile).reshape(NZ, 16, SEQ)
            return carry

        lax.fori_loop(0, 2 * NX, block, 0)

    @pl.when(sec < 3)
    def _():
        relay(0, 0)

    @pl.when(s0 == 0)
    def _():
        relay(1, 0)
        relay(0, 1)
        relay(1, 1)
        turn_weights()
        turn(0)
        turn(1)

    def backward(m, carry):
        @pl.when(sec < 3)
        def _():
            g_copy(m).wait_recv()

        scale = mods[pl.ds(m, 1), pl.ds(D, D)]
        gate = mods[pl.ds(m, 1), pl.ds(2 * D, D)]
        pc_scr[m] = (gate * g_scr[m].astype(F32)).astype(BF16)

        @pl.when(s0 == 0)
        def _():
            for copy in cot_copies(m, 2):
                copy.start()

        for n in range(2):
            cols = pl.ds(n * 512, 512)
            datt_scr[:, cols] = dot_nn(pc_scr[m], wout_t[:, cols]).astype(BF16)

        def pair(j):
            cq, ck, cv = lanes(j * 128, 128), lanes(D + j * 128, 128), lanes(2 * D + j * 128, 128)
            q2 = both(qkv_scr[m, :, cq])
            k = qkv_scr[m, :, ck]
            v = qkv_scr[m, :, cv]
            do2 = both(datt_scr[:, cq])
            p = p_scr[m, j]
            dv = dot_tn(p.astype(BF16), do2)
            dp = dot_nt(do2, v).astype(BF16).astype(F32)
            ds = p * (dp - jnp.sum(dp * p, axis=-1, keepdims=True))
            ds = (ds * (1.0 / math.sqrt(HEAD_DIM))).astype(BF16)
            dqkv_scr[m, :, cv] = dv.astype(BF16)
            dqkv_scr[m, :, cq] = merged(dot_nn(ds, k)).astype(BF16)
            dqkv_scr[m, :, ck] = dot_tn(ds, q2).astype(BF16)

        over_pairs(pair)
        for k in (3, 4, 5):
            for copy in cot_copies(m, k):
                copy.start()

        @pl.when(sec > 0)
        def _():
            for n in range(2):
                cols = pl.ds(n * 512, 512)
                tmp_scr[:, cols] = dot_nn(dqkv_scr[m], wqkv_t[:, cols]).astype(BF16)
            hf = h_scr[m].astype(F32)
            r = r_scr[m][:, :1]
            u = tmp_scr[...].astype(F32) * (1.0 + scale)
            inner = jnp.sum(u * hf, axis=-1, keepdims=True) * (1.0 / D)
            dh = (u * r - hf * (r * r * r * inner)).astype(BF16).astype(F32)
            gs_scr[m] = (dh + g_scr[m].astype(F32)).astype(BF16)
            g_copy(m).start()

        rows = rows_of(mx, m)
        ball[rows] = dqkv_scr[m, :, lanes(mx * QB, QB)]
        pall[rows] = pc_scr[m, :, lanes(mx * OB, OB)]

        @pl.when((sec == 2) & (m == 0))
        def _():
            relay(1, 0)

        return carry

    lax.fori_loop(0, 2, backward, 0)

    @pl.when(sec == 3)
    def _():
        relay(0, 0)
        relay(1, 0)

    def exchanged(quarter):
        def arrive(m, carry):
            for copy in cot_copies(m, 2 + quarter):
                copy.wait_recv()
            return carry

        lax.fori_loop(0, 2, arrive, 0)

    def partial(quarter):
        def of(dest):
            left = (n_t if quarter else a_t)[:, dest].reshape(8 * 16, NX * 2 * SEQ)
            if quarter == 0:
                return dot_nn(left, pall[...])
            return dot_nn(left, ball[:, pl.ds((quarter - 1) * OB, OB)])

        return of

    def wide(c):
        def of(dest):
            left = a_t[:, dest, :, pl.ds(0, 2 * SEQ)].reshape(8 * 16, 2 * SEQ)
            return dot_nn(left, pc_scr[:, :, pl.ds(c * OB, OB)].reshape(2 * SEQ, OB))

        return of

    def wide_ring(c):
        return 3 + c if c else 0

    z_up = {"dp_2": lax.rem(mz + 1, NZ)}
    z_dn = {"dp_2": lax.rem(mz + NZ - 1, NZ)}

    def ring_copy(up, t, quarter):
        k = 4 * quarter + t
        if up:
            return remote(up_out.at[k], up_in.at[k], up_send.at[k], up_recv.at[k], z_up)
        return remote(dn_out.at[k], dn_in.at[k], dn_send.at[k], dn_recv.at[k], z_dn)

    def hops(up, quarter):
        return 4 if up == (quarter % 2 == 0) else 3

    def y_copy(quarter):
        return remote(
            y_out.at[quarter], y_in.at[quarter], y_send.at[quarter], y_recv.at[quarter], partner
        )

    def ring_step(t, ring, part):
        for up in (True, False):
            n = hops(up, ring)
            if t >= n:
                continue
            out, got = (up_out, up_in) if up else (dn_out, dn_in)
            val = part(lax.rem(mz + NZ + (n - t if up else t - n), NZ))
            if t > 0:
                ring_copy(up, t - 1, ring).wait_recv()
                val = val + got[4 * ring + t - 1].astype(F32)
            out[4 * ring + t] = val.astype(BF16)
            ring_copy(up, t, ring).start()

    def ring_sum(ring, part):
        val = part(mz)
        for up in (True, False):
            n = hops(up, ring)
            ring_copy(up, n - 1, ring).wait_recv()
            val = val + (up_in if up else dn_in)[4 * ring + n - 1].astype(F32)
        return val

    def ring_end(quarter, val):
        summed[quarter] = val.reshape(2, NX * 16, OB)
        y_out[quarter] = summed[quarter, 1 - d0].astype(BF16)
        y_copy(quarter).start()

    def c_copy(d):
        to = lax.rem(mx + d, NX)
        return remote(
            c_out.at[to], c_in.at[d - 1], c_send.at[d - 1], c_recv.at[d - 1], {"dp_1": to}
        )

    def o_copies(quarter):
        made = []
        for i, where in enumerate(x_peers):
            if quarter == 0:
                src, dst = toto.at[where["dp_1"]], outo_ref.at[:, lanes(mx * OB, OB)]
            else:
                src = totq.at[quarter - 1, where["dp_1"]]
                dst = outq_ref.at[:, lanes(mx * QB + (quarter - 1) * OB, OB)]
            made.append(remote(src, dst, o_send.at[quarter, i], o_recv.at[quarter, i], where))
        return made

    def y_end(quarter, acc):
        y_copy(quarter).wait_recv()
        full = summed[quarter, d0] + y_in[quarter].astype(F32)
        by_x = full.reshape(NX, 16, OB)
        if quarter == 0:
            toto[...] = by_x
        else:
            totq[quarter - 1] = by_x
        for copy in o_copies(quarter):
            copy.start()
        full = full * full
        for c in range(2):
            for i in range(NX * 2):
                acc = acc + full[i * 8 : (i + 1) * 8, c * 128 : (c + 1) * 128]
        return acc

    @pl.when(s0 == 0)
    def _():
        exchanged(0)
        for t in range(4):
            ring_step(t, 0, partial(0))
        ring_end(0, ring_sum(0, partial(0)))

    @pl.when(s0 == 1)
    def _():
        for m in range(2):
            for g in range(8):
                tile = att_scr[m, :, pl.ds(g * 128, 128)]
                a_t[g, :, :, pl.ds(m * SEQ, SEQ)] = jnp.transpose(tile).reshape(NZ, 16, SEQ)
        for t in range(4):
            for c in range(NX):
                ring_step(t, wide_ring(c), wide(c))
        for c in range(NX):
            c_sum[c] = ring_sum(wide_ring(c), wide(c))
            c_out[c] = c_sum[c].astype(BF16)
        for d in range(1, NX):
            c_copy(d).start()
        turn(0)

    for t in range(4):
        for quarter in range(1, 4):
            if t == 0:
                exchanged(quarter)
            ring_step(t, quarter, partial(quarter))

    @pl.when(s0 == 1)
    def _():
        val = c_sum[mx]
        for d in range(1, NX):
            c_copy(d).wait_recv()
            val = val + c_in[d - 1].astype(F32)
        ring_end(0, val)

    for quarter in range(1, 4):
        ring_end(quarter, ring_sum(quarter, partial(quarter)))
    acc = jnp.zeros((8, 128), F32)
    for quarter in range(4):
        acc = y_end(quarter, acc)
    sqs[0] = acc

    def sum_over(peers, src, buf, ssem, rsem):
        copies = [
            remote(src, buf.at[i], ssem.at[i], rsem.at[i], where) for i, where in enumerate(peers)
        ]
        for copy in copies:
            copy.start()
        return copies

    def take(copies, src, buf):
        for copy in copies:
            copy.wait_recv()
        acc = src[...]
        for i in range(len(copies)):
            acc = acc + buf[i]
        return acc

    qz = sum_over(z_peers, sqs.at[0], sqz, qz_send, qz_recv)
    outo_ref[:, lanes(mx * OB, OB)] = toto[mx]
    for quarter in range(1, 4):
        outq_ref[:, lanes(mx * QB + (quarter - 1) * OB, OB)] = totq[quarter - 1, mx]
    sqs[1] = take(qz, sqs.at[0], sqz)
    qx = sum_over(x_peers, sqs.at[1], sqx, qx_send, qx_recv)
    sqs[2] = take(qx, sqs.at[1], sqx)
    qr = sum_over(r_peers, sqs.at[2], sqr, qr_send, qr_recv)
    total = take(qr, sqs.at[2], sqr)
    total = jnp.sum(jnp.sum(total, axis=1, keepdims=True), axis=0, keepdims=True)
    factor_ref[...] = jnp.broadcast_to(lax.rsqrt(total / 16777216.0 + 1e-12), (8, 128))
    for quarter in range(4):
        for copy in o_copies(quarter):
            copy.wait_recv()
    def ring_sent(ring):
        for up in (True, False):
            for t in range(hops(up, ring)):
                ring_copy(up, t, ring).wait_send()

    for quarter in range(4):
        ring_sent(quarter)
        y_copy(quarter).wait_send()
        for copy in o_copies(quarter):
            copy.wait_send()

    @pl.when(s0 == 1)
    def _():
        for c in range(1, NX):
            ring_sent(wide_ring(c))
            c_copy(c).wait_send()

    for copy in qz + qx + qr:
        copy.wait_send()

    def finish(m, carry):
        for copy in act_copies(m, 0) + [relay_copy(m, 0)]:
            copy.wait_send()
        for k in (3, 4, 5):
            for copy in cot_copies(m, k):
                copy.wait_send()

        @pl.when(s0 == 0)
        def _():
            for copy in act_copies(m, 1) + [relay_copy(m, 1)] + cot_copies(m, 2):
                copy.wait_send()

        @pl.when(sec < 3)
        def _():
            h_copy(m, 0).wait_send()
            h_copy(m, 1).wait_send()

        @pl.when(sec > 0)
        def _():
            g_copy(m).wait_send()

        return carry

    lax.fori_loop(0, 2, finish, 0)

    @pl.when(s0 == 1)
    def _():
        swap_mod().wait_send()
        swap_noise().wait_send()


def run_step(h0, mod, noise, w_qkv, w_out, head):
    shape = jax.ShapeDtypeStruct
    dma = pltpu.SemaphoreType.DMA
    vmem = pltpu.VMEM
    rows = NX * 2 * SEQ
    return pl.pallas_call(
        step_kernel,
        out_shape=(shape((16, 3 * D), F32), shape((16, D), F32), shape((8, 128), F32)),
        in_specs=[VMEM, VMEM, VMEM, ANY, ANY, VMEM],
        out_specs=[VMEM] * 3,
        scratch_shapes=[
            vmem((D, 3 * D), BF16),
            vmem((D, D), BF16),
            vmem((3 * D, D), BF16),
            vmem((D, D), BF16),
            vmem((rows, D), BF16),
            vmem((rows, D), BF16),
            vmem((rows, QB), BF16),
            vmem((rows, OB), BF16),
            vmem((8, NZ, 16, rows), BF16),
            vmem((8, NZ, 16, rows), BF16),
            vmem((2, SEQ, D), BF16),
            vmem((2, SEQ, D), BF16),
            vmem((2, SEQ, D), BF16),
            vmem((2, SEQ, D), BF16),
            vmem((2, SEQ, 3 * D), BF16),
            vmem((2, HEADS // 2, 2 * SEQ, SEQ), F32),
            vmem((2, SEQ, 128), F32),
            vmem((2, SEQ, D), BF16),
            vmem((2, SEQ, D), BF16),
            vmem((2, SEQ, 3 * D), BF16),
            vmem((2, SEQ, D), BF16),
            vmem((SEQ, D), BF16),
            vmem((SEQ, D), BF16),
            vmem((8, 3 * D), F32),
            vmem((2, 16, SEQ), F32),
            vmem((28, 128, OB), BF16),
            vmem((28, 128, OB), BF16),
            vmem((28, 128, OB), BF16),
            vmem((28, 128, OB), BF16),
            vmem((NX, 128, OB), F32),
            vmem((NX, 128, OB), BF16),
            vmem((NX - 1, 128, OB), BF16),
            vmem((4, 2, NX * 16, OB), F32),
            vmem((4, NX * 16, OB), BF16),
            vmem((4, NX * 16, OB), BF16),
            vmem((3, NX, 16, OB), F32),
            vmem((NX, 16, OB), F32),
            vmem((3, 8, 128), F32),
            vmem((NZ - 1, 8, 128), F32),
            vmem((NX - 1, 8, 128), F32),
            vmem((7, 8, 128), F32),
            dma((2, 2)), dma((2, 2)), dma((2,)), dma((2,)), dma((2,)), dma((2,)),
            dma((2, NX - 1, 6)), dma((2, NX - 1, 6)),
            dma((28,)), dma((28,)), dma((28,)), dma((28,)), dma((NX - 1,)), dma((NX - 1,)),
            dma((4,)), dma((4,)),
            dma((4, NX - 1)), dma((4, NX - 1)),
            dma((NZ - 1,)), dma((NZ - 1,)), dma((NX - 1,)), dma((NX - 1,)), dma((7,)), dma((7,)),
            dma((2,)),
        ],
        compiler_params=pltpu.CompilerParams(
            collective_id=0, has_side_effects=True, vmem_limit_bytes=58 * 2**20
        ),
        name="step",
    )(h0, mod, noise, w_qkv, w_out, head)


def optimizer_kernel(gq, go, factor_ref, mq, mo, vq, vo, uq, uo, nmq, nmo, nvq, nvo):
    factor = factor_ref[0:1, 0:1]
    for g, m, v, u, nm, nv in ((gq, mq, vq, uq, nmq, nvq), (go, mo, vo, uo, nmo, nvo)):
        normalized = g[...] * factor
        moment = 0.9 * m[0] + 0.1 * normalized
        second = 0.99 * v[0] + 0.01 * normalized * normalized
        u[0] = moment / (jnp.sqrt(second) + 1e-08)
        nm[0] = moment
        nv[0] = second


def optimizer(gq, go, factor, mq, mo, vq, vo):
    shape = jax.ShapeDtypeStruct
    big, small = shape((1, 16, 3 * D), F32), shape((1, 16, D), F32)
    return pl.pallas_call(
        optimizer_kernel,
        out_shape=(big, small, big, small, big, small),
        in_specs=[VMEM] * 7,
        out_specs=[VMEM] * 6,
        name="optimizer",
    )(gq, go, factor, mq, mo, vq, vo)


def local(
    latents,
    noise,
    timesteps,
    cameras,
    embed_in,
    camera_table,
    w_mod,
    w_qkv,
    w_out,
    head_out,
    moment_qkv,
    moment_out,
    second_qkv,
    second_out,
):
    time_emb = time_embed(timesteps, w_mod.shape[1])
    time_rows = jnp.pad(time_emb, ((0, 6), (0, 0)))
    mod = jnp.dot(time_rows, w_mod[0], preferred_element_type=jnp.float32)
    h0 = jax.vmap(embed_sample, in_axes=(0, 0, 0, 0, None, None))(
        latents, noise, timesteps, cameras, embed_in, camera_table
    )
    noise_rows = jnp.pad(noise.astype(F32), ((0, 0), (0, 12), (0, 0)))
    head = jnp.pad(head_out, ((0, 12), (0, 0)))
    qkv_rows, out_rows, factors = run_step(h0, mod, noise_rows, w_qkv[0], w_out[0], head)
    return optimizer(
        qkv_rows, out_rows, factors, moment_qkv, moment_out, second_qkv, second_out
    )


def solution(mesh):
    torus = Mesh(
        mesh.devices.reshape(2, 2, 2, 4, 8), ("section_0", "section_1", "dp_0", "dp_1", "dp_2")
    )
    return jax.shard_map(
        local,
        mesh=torus,
        in_specs=(
            P(DP, None, None),
            P(DP, None, None),
            P(DP),
            P(DP, None),
            P(),
            P(),
            P(SECTION, None, None),
            P(SECTION, None, None),
            P(SECTION, None, None),
            P(),
            P(SECTION, DP, None),
            P(SECTION, DP, None),
            P(SECTION, DP, None),
            P(SECTION, DP, None),
        ),
        out_specs=(
            P(SECTION, DP, None),
            P(SECTION, DP, None),
            P(SECTION, DP, None),
            P(SECTION, DP, None),
            P(SECTION, DP, None),
            P(SECTION, DP, None),
        ),
        check_vma=False,
    )
```

```python
import functools
import math

import jax
import jax.numpy as jnp
from jax import lax
from jax.experimental import pallas as pl
from jax.experimental.pallas import tpu as pltpu
from jax.sharding import Mesh
from jax.sharding import PartitionSpec as P

HEADS = 16
HEAD_DIM = 64
SECTION = ("section_0", "section_1")
DP = ("dp_0", "dp_1", "dp_2")
MESH = pl.DeviceIdType.MESH
F32 = jnp.float32
BF16 = jnp.bfloat16
D = 1024
SEQ = 128
NX = 4
NZ = 8
QB = 3 * D // NX
OB = D // NX
VMEM = pl.BlockSpec(memory_space=pltpu.VMEM)
ANY = pl.BlockSpec(memory_space=pl.ANY)


def time_embed(step_ids, emb_width):
    half_dim = emb_width // 2
    frequency = jnp.exp(-math.log(10000.0) * jnp.arange(half_dim, dtype=jnp.float32) / half_dim)
    phases = step_ids.astype(jnp.float32)[:, None] * frequency[None, :]
    joined = jnp.concatenate([jnp.cos(phases), jnp.sin(phases)], axis=-1)
    return jax.nn.silu(joined).astype(jnp.bfloat16)


def embed_sample(latent_now, noise_now, step_now, camera_now, embed_in, camera_table):
    step_f = step_now.astype(jnp.float32)
    alpha_bar = jnp.cos((step_f / 1000.0 + 0.008) / 1.008 * (math.pi / 2.0)) ** 2
    noised = jnp.sqrt(alpha_bar) * latent_now.astype(jnp.float32) + jnp.sqrt(
        1.0 - alpha_bar
    ) * noise_now.astype(jnp.float32)
    features = lax.dot_general(
        noised.astype(jnp.bfloat16),
        embed_in,
        (((0,), (0,)), ((), ())),
        preferred_element_type=jnp.float32,
    )
    onehot = (
        camera_now[:, None] == jnp.arange(camera_table.shape[0], dtype=jnp.int32)[None, :]
    ).astype(jnp.bfloat16)
    camera_vec = jnp.dot(onehot, camera_table, preferred_element_type=jnp.float32)
    model_width = embed_in.shape[1]
    views = camera_now.shape[0]
    joined = features.reshape(views, -1, model_width) + camera_vec[:, None, :]
    return joined.reshape(-1, model_width).astype(jnp.bfloat16)


def dot_nn(a, b):
    return lax.dot_general(a, b, (((1,), (0,)), ((), ())), preferred_element_type=F32)


def dot_nt(a, b):
    return lax.dot_general(a, b, (((1,), (1,)), ((), ())), preferred_element_type=F32)


def dot_tn(a, b):
    return lax.dot_general(a, b, (((0,), (0,)), ((), ())), preferred_element_type=F32)


def lanes(start, size):
    return pl.ds(pl.multiple_of(start, 128), size)


def step_kernel(
    h0_ref, mod_ref, noise_ref, wqkv_hbm, wout_hbm, head_ref,
    outq_ref, outo_ref, factor_ref,
    wqkv_ref, wout_ref, wqkv_t, wout_t, nall, aall, ball, pall, n_t, a_t,
    h_scr, hn_scr, nrm_scr, att_scr, qkv_scr, p_scr, r_scr, g_scr, gs_scr,
    dqkv_scr, pc_scr, datt_scr, tmp_scr, mods, noi,
    up_out, up_in, dn_out, dn_in, c_sum, c_out, c_in, share, summed, y_out, y_in, totq, toto, sqs, sqz, sqp,
    h_send, h_recv, g_send, g_recv, sw_send, sw_recv, x_send, x_recv,
    up_send, up_recv, dn_send, dn_recv, c_send, c_recv, y_send, y_recv, o_send, o_recv,
    qz_send, qz_recv, qp_send, qp_recv, w_sem,
):
    w_copies = [
        pltpu.make_async_copy(wqkv_hbm, wqkv_ref, w_sem.at[0]),
        pltpu.make_async_copy(wout_hbm, wout_ref, w_sem.at[1]),
    ]
    for copy in w_copies:
        copy.start()
    s0 = lax.axis_index("section_0")
    s1 = lax.axis_index("section_1")
    d0 = lax.axis_index("dp_0")
    mx = lax.axis_index("dp_1")
    mz = lax.axis_index("dp_2")
    sec = 2 * s0 + s1

    def toward(step):
        other = sec + step
        o0 = lax.rem(lax.div(other + 4, 2), 2)
        o1 = lax.rem(other + 4, 2)
        crossing = (o0 + s0) - 2 * o0 * s0
        od = (d0 + crossing) - 2 * d0 * crossing
        return {"section_0": o0, "section_1": o1, "dp_0": od}

    nxt = toward(1)
    prv = toward(-1)
    partner = {"dp_0": 1 - d0}

    barrier = pltpu.get_barrier_semaphore()

    def greet(where):
        pl.semaphore_signal(barrier, inc=1, device_id=where, device_id_type=MESH)

    def flip(a, by):
        return 1 - a if by else a

    z_peers = [{"dp_2": lax.rem(mz + d, NZ)} for d in range(1, NZ)]
    x_peers = [{"dp_1": lax.rem(mx + d, NX)} for d in range(1, NX)]
    plane = [
        {
            "section_0": flip(s0, c & 4),
            "section_1": flip(s1, c & 2),
            "dp_0": flip(d0, c & 1),
            "dp_1": lax.rem(mx + c // 8, NX),
        }
        for c in range(1, 32)
    ]
    for where in z_peers + plane:
        greet(where)

    @pl.when(sec < 3)
    def _():
        greet(nxt)

    @pl.when(sec > 0)
    def _():
        greet(prv)

    pl.semaphore_wait(barrier, 38 + lax.min(sec, 1) + lax.min(3 - sec, 1))

    def remote(src, dst, ssem, rsem, where):
        return pltpu.make_async_remote_copy(
            src_ref=src, dst_ref=dst, send_sem=ssem, recv_sem=rsem,
            device_id=where, device_id_type=MESH,
        )

    def swap_mod():
        return remote(mod_ref, mods, sw_send.at[0], sw_recv.at[0], partner)

    def swap_noise():
        return remote(noise_ref, noi, sw_send.at[1], sw_recv.at[1], partner)

    @pl.when(s0 == 1)
    def _():
        swap_mod().start()
        swap_noise().start()
        swap_mod().wait_recv()
        swap_noise().wait_recv()

    @pl.when(s0 == 0)
    def _():
        mods[...] = mod_ref[...]

    def h_copy(m, n):
        cols = pl.ds(n * 512, 512)
        return remote(
            hn_scr.at[m, :, cols], h_scr.at[m, :, cols], h_send.at[m, n], h_recv.at[m, n], nxt
        )

    def g_copy(m):
        return remote(gs_scr.at[m], g_scr.at[m], g_send.at[m], g_recv.at[m], prv)

    def rows_of(src, m):
        return pl.ds(pl.multiple_of(src * 2 * SEQ + m * SEQ, SEQ), SEQ)

    def x_copy(m, d, k):
        to = lax.rem(mx + d, NX)
        rows = rows_of(mx, m)
        src, dst = (
            (nrm_scr.at[m], nall.at[rows]),
            (att_scr.at[m], aall.at[rows]),
            (pc_scr.at[m, :, lanes(to * OB, OB)], pall.at[rows]),
        )[k] if k < 3 else (
            dqkv_scr.at[m, :, lanes(to * QB + (k - 3) * OB, OB)],
            ball.at[rows, pl.ds((k - 3) * OB, OB)],
        )
        return remote(src, dst, x_send.at[m, d - 1, k], x_recv.at[m, d - 1, k], {"dp_1": to})

    def act_copies(m, k):
        return [x_copy(m, d, k) for d in (1, 3)]

    def cot_copies(m, k):
        return [x_copy(m, d, k) for d in (1, 2, 3)]

    def relay_copy(m, k):
        by = 1 if k == 0 else 3
        rows = rows_of(lax.rem(mx + NX - by, NX), m)
        held = (nall, aall)[k].at[rows]
        return remote(
            held, held, x_send.at[m, 1, k], x_recv.at[m, 1, k], {"dp_1": lax.rem(mx + by, NX)}
        )

    def relay(m, k):
        x_copy(m, 1 if k == 0 else 3, k).wait_recv()
        relay_copy(m, k).start()

    low = lax.broadcasted_iota(jnp.int32, (SEQ, 128), 1) < HEAD_DIM

    def both(tile):
        zero = jnp.zeros_like(tile)
        return jnp.concatenate([jnp.where(low, tile, zero), jnp.where(low, zero, tile)], axis=0)

    def merged(pair):
        return jnp.where(low, pair[:SEQ], pair[SEQ:])

    PAIRS = HEADS // 2
    GROUP = 8

    def over_pairs(body):
        def step(i, carry):
            for j in range(GROUP):
                body(i * GROUP + j)
            return carry

        lax.fori_loop(0, PAIRS // GROUP, step, 0)

    def forward(m, carry):
        @pl.when(sec == 0)
        def _():
            h_scr[m] = h0_ref[m]

        @pl.when(sec > 0)
        def _():
            h_copy(m, 0).wait_recv()
            h_copy(m, 1).wait_recv()

        shift = mods[pl.ds(m, 1), pl.ds(0, D)]
        scale = mods[pl.ds(m, 1), pl.ds(D, D)]
        gate = mods[pl.ds(m, 1), pl.ds(2 * D, D)]
        hf = h_scr[m].astype(F32)
        r = lax.rsqrt(jnp.mean(hf * hf, axis=-1, keepdims=True) + 1e-06)
        r_scr[m] = jnp.broadcast_to(r, (SEQ, 128))
        nrm_scr[m] = (hf * r * (1.0 + scale) + shift).astype(BF16)
        for n in range(6):
            cols = pl.ds(n * 512, 512)
            qkv_scr[m, :, cols] = dot_nn(nrm_scr[m], wqkv_ref[:, cols]).astype(BF16)

        def pair(j):
            q = qkv_scr[m, :, lanes(j * 128, 128)]
            k = qkv_scr[m, :, lanes(D + j * 128, 128)]
            v = qkv_scr[m, :, lanes(2 * D + j * 128, 128)]
            s = dot_nt(both(q), k) * (1.0 / math.sqrt(HEAD_DIM))
            s = jnp.exp(s - jnp.max(s, axis=-1, keepdims=True))
            p = s / jnp.sum(s, axis=-1, keepdims=True)
            p_scr[m, j] = p
            att_scr[m, :, lanes(j * 128, 128)] = merged(dot_nn(p.astype(BF16), v)).astype(BF16)

        over_pairs(pair)
        for n in range(2):
            cols = pl.ds(n * 512, 512)
            proj = dot_nn(att_scr[m], wout_ref[:, cols])
            hn_scr[m, :, cols] = (
                h_scr[m, :, cols].astype(F32) + gate[:, n * 512 : (n + 1) * 512] * proj
            ).astype(BF16)

            @pl.when(sec < 3)
            def _():
                h_copy(m, n).start()

        for copy in act_copies(m, 0):
            copy.start()
        rows = rows_of(mx, m)
        nall[rows] = nrm_scr[m]

        @pl.when(sec == 4)
        def _():
            for copy in act_copies(m, 1):
                copy.start()
            aall[rows] = att_scr[m]

        @pl.when(sec == 3)
        def _():
            ff = hn_scr[m].astype(F32)
            rr = lax.rsqrt(jnp.mean(ff * ff, axis=-1, keepdims=True) + 1e-06)
            predicted = dot_nt(head_ref[...], (ff * rr).astype(BF16))
            err = 2.0 * (predicted - noi[m].astype(F32))
            hi = err.astype(BF16)
            lo = (err - hi.astype(F32)).astype(BF16)
            dn = (dot_tn(hi, head_ref[...]) + dot_tn(lo, head_ref[...])).astype(BF16).astype(F32)
            inner = jnp.sum(dn * ff, axis=-1, keepdims=True) * (1.0 / D)
            g_scr[m] = (dn * rr - ff * (rr * rr * rr * inner)).astype(BF16)

        return carry

    def turn_weights():
        def block(i, carry):
            here = lanes(i * 128, 128)
            for src, dst, tiles in ((wqkv_ref, wqkv_t, 24), (wout_ref, wout_t, 8)):
                for g in range(tiles):
                    dst[pl.ds(g * 128, 128), here] = jnp.transpose(src[here, pl.ds(g * 128, 128)])
            return carry

        lax.fori_loop(0, 8, block, 0)

    for copy in w_copies:
        copy.wait()

    @pl.when(s0 == 1)
    def _():
        turn_weights()

    lax.fori_loop(0, 2, forward, 0)

    def turn(k):
        def arrived(m, carry):
            x_copy(m, 3 if k == 0 else 1, k).wait_recv()
            relay_copy(m, k).wait_recv()
            return carry

        lax.fori_loop(0, 2, arrived, 0)

        def block(i, carry):
            here = lanes(i * SEQ, SEQ)
            src, dst = ((nall, n_t), (aall, a_t))[k]
            for g in range(8):
                tile = src[here, pl.ds(g * 128, 128)]
                dst[g, :, :, here] = jnp.transpose(tile).reshape(NZ, 16, SEQ)
            return carry

        lax.fori_loop(0, 2 * NX, block, 0)

    @pl.when(sec < 3)
    def _():
        relay(0, 0)

    @pl.when(s0 == 0)
    def _():
        relay(1, 0)
        turn_weights()
        turn(0)

    @pl.when(sec == 4)
    def _():
        relay(0, 1)
        relay(1, 1)
        turn(1)

    def backward(m, carry):
        @pl.when(sec < 3)
        def _():
            g_copy(m).wait_recv()

        scale = mods[pl.ds(m, 1), pl.ds(D, D)]
        gate = mods[pl.ds(m, 1), pl.ds(2 * D, D)]
        pc_scr[m] = (gate * g_scr[m].astype(F32)).astype(BF16)

        @pl.when(sec == 4)
        def _():
            for copy in cot_copies(m, 2):
                copy.start()

        for n in range(2):
            cols = pl.ds(n * 512, 512)
            datt_scr[:, cols] = dot_nn(pc_scr[m], wout_t[:, cols]).astype(BF16)

        def pair(j):
            cq, ck, cv = lanes(j * 128, 128), lanes(D + j * 128, 128), lanes(2 * D + j * 128, 128)
            q2 = both(qkv_scr[m, :, cq])
            k = qkv_scr[m, :, ck]
            v = qkv_scr[m, :, cv]
            do2 = both(datt_scr[:, cq])
            p = p_scr[m, j]
            dv = dot_tn(p.astype(BF16), do2)
            dp = dot_nt(do2, v).astype(BF16).astype(F32)
            ds = p * (dp - jnp.sum(dp * p, axis=-1, keepdims=True))
            ds = (ds * (1.0 / math.sqrt(HEAD_DIM))).astype(BF16)
            dqkv_scr[m, :, cv] = dv.astype(BF16)
            dqkv_scr[m, :, cq] = merged(dot_nn(ds, k)).astype(BF16)
            dqkv_scr[m, :, ck] = dot_tn(ds, q2).astype(BF16)

        over_pairs(pair)
        for k in (3, 4, 5):
            for copy in cot_copies(m, k):
                copy.start()

        @pl.when(sec > 0)
        def _():
            for n in range(2):
                cols = pl.ds(n * 512, 512)
                tmp_scr[:, cols] = dot_nn(dqkv_scr[m], wqkv_t[:, cols]).astype(BF16)
            hf = h_scr[m].astype(F32)
            r = r_scr[m][:, :1]
            u = tmp_scr[...].astype(F32) * (1.0 + scale)
            inner = jnp.sum(u * hf, axis=-1, keepdims=True) * (1.0 / D)
            dh = (u * r - hf * (r * r * r * inner)).astype(BF16).astype(F32)
            gs_scr[m] = (dh + g_scr[m].astype(F32)).astype(BF16)
            g_copy(m).start()

        rows = rows_of(mx, m)
        ball[rows] = dqkv_scr[m, :, lanes(mx * QB, QB)]
        pall[rows] = pc_scr[m, :, lanes(mx * OB, OB)]

        @pl.when((sec == 2) & (m == 0))
        def _():
            relay(1, 0)

        return carry

    lax.fori_loop(0, 2, backward, 0)

    @pl.when(sec == 3)
    def _():
        relay(0, 0)
        relay(1, 0)

    def exchanged(quarter):
        def arrive(m, carry):
            for copy in cot_copies(m, 2 + quarter):
                copy.wait_recv()
            return carry

        lax.fori_loop(0, 2, arrive, 0)

    def multiply(ring, left_of, right_of):
        def rows(i, carry):
            val = dot_nn(left_of(i), right_of())
            share[ring, pl.ds(2 * i, 2)] = val.reshape(2, NZ, 16, OB)
            return carry

        lax.fori_loop(0, 4, rows, 0)

    def multiply_all(quarter):
        src = n_t if quarter else a_t

        def left(i):
            return src[pl.ds(2 * i, 2)].reshape(256, NX * 2 * SEQ)

        def right():
            return ball[:, pl.ds((quarter - 1) * OB, OB)] if quarter else pall[...]

        multiply(quarter, left, right)

    def multiply_own(c):
        def left(i):
            return a_t[pl.ds(2 * i, 2), :, :, pl.ds(0, 2 * SEQ)].reshape(256, 2 * SEQ)

        def right():
            return pc_scr[:, :, pl.ds(c * OB, OB)].reshape(2 * SEQ, OB)

        multiply(wide_ring(c), left, right)

    def part(ring, dest):
        return share[ring, :, dest].reshape(128, OB)

    def wide_ring(c):
        return 3 + c if c else 0

    z_up = {"dp_2": lax.rem(mz + 1, NZ)}
    z_dn = {"dp_2": lax.rem(mz + NZ - 1, NZ)}

    def ring_copy(up, t, quarter):
        k = 4 * quarter + t
        if up:
            return remote(up_out.at[k], up_in.at[k], up_send.at[k], up_recv.at[k], z_up)
        return remote(dn_out.at[k], dn_in.at[k], dn_send.at[k], dn_recv.at[k], z_dn)

    def hops(up, quarter):
        return 4 if up == (quarter % 2 == 0) else 3

    def y_copy(quarter):
        return remote(
            y_out.at[quarter], y_in.at[quarter], y_send.at[quarter], y_recv.at[quarter], partner
        )

    def ring_step(t, ring):
        for up in (True, False):
            n = hops(up, ring)
            if t >= n:
                continue
            out, got = (up_out, up_in) if up else (dn_out, dn_in)
            val = part(ring, lax.rem(mz + NZ + (n - t if up else t - n), NZ))
            if t > 0:
                ring_copy(up, t - 1, ring).wait_recv()
                val = val + got[4 * ring + t - 1].astype(F32)
            out[4 * ring + t] = val.astype(BF16)
            ring_copy(up, t, ring).start()

    def ring_sum(ring):
        val = part(ring, mz)
        for up in (True, False):
            n = hops(up, ring)
            ring_copy(up, n - 1, ring).wait_recv()
            val = val + (up_in if up else dn_in)[4 * ring + n - 1].astype(F32)
        return val

    def ring_end(quarter, val):
        summed[quarter] = val.reshape(2, NX * 16, OB)
        y_out[quarter] = summed[quarter, 1 - d0].astype(BF16)
        y_copy(quarter).start()

    def c_copy(d):
        to = lax.rem(mx + d, NX)
        return remote(
            c_out.at[to], c_in.at[d - 1], c_send.at[d - 1], c_recv.at[d - 1], {"dp_1": to}
        )

    def o_copies(quarter):
        made = []
        for i, where in enumerate(x_peers):
            if quarter == 0:
                src, dst = toto.at[where["dp_1"]], outo_ref.at[:, lanes(mx * OB, OB)]
            else:
                src = totq.at[quarter - 1, where["dp_1"]]
                dst = outq_ref.at[:, lanes(mx * QB + (quarter - 1) * OB, OB)]
            made.append(remote(src, dst, o_send.at[quarter, i], o_recv.at[quarter, i], where))
        return made

    def y_end(quarter, acc):
        y_copy(quarter).wait_recv()
        full = summed[quarter, d0] + y_in[quarter].astype(F32)
        by_x = full.reshape(NX, 16, OB)
        if quarter == 0:
            toto[...] = by_x
        else:
            totq[quarter - 1] = by_x
        for copy in o_copies(quarter):
            copy.start()
        full = full * full
        for c in range(2):
            for i in range(NX * 2):
                acc = acc + full[i * 8 : (i + 1) * 8, c * 128 : (c + 1) * 128]
        return acc

    def own_shares():
        for m in range(2):
            for g in range(8):
                tile = att_scr[m, :, pl.ds(g * 128, 128)]
                a_t[g, :, :, pl.ds(m * SEQ, SEQ)] = jnp.transpose(tile).reshape(NZ, 16, SEQ)
        for c in range(NX):
            multiply_own(c)
            ring_step(0, wide_ring(c))

    def own_steps(t):
        for c in range(NX):
            ring_step(t, wide_ring(c))

    def own_sums():
        for c in range(NX):
            c_sum[c] = ring_sum(wide_ring(c))
            c_out[c] = c_sum[c].astype(BF16)
        for d in range(1, NX):
            c_copy(d).start()

    @pl.when(sec == 4)
    def _():
        exchanged(0)
        multiply_all(0)
        ring_step(0, 0)

    own_shares()

    @pl.when(s0 == 1)
    def _():
        for t in range(1, 4):
            own_steps(t)
        own_sums()
        turn(0)

    for quarter in range(1, 4):
        exchanged(quarter)
        multiply_all(quarter)
        ring_step(0, quarter)
    for t in range(1, 4):
        @pl.when(sec == 4)
        def _():
            ring_step(t, 0)

        @pl.when(s0 == 0)
        def _():
            own_steps(t)

        for quarter in range(1, 4):
            ring_step(t, quarter)

    @pl.when(sec == 4)
    def _():
        ring_end(0, ring_sum(0))

    @pl.when(s0 == 0)
    def _():
        own_sums()

    for quarter in range(1, 4):
        ring_end(quarter, ring_sum(quarter))

    @pl.when(sec < 4)
    def _():
        val = c_sum[mx]
        for d in range(1, NX):
            c_copy(d).wait_recv()
            val = val + c_in[d - 1].astype(F32)
        ring_end(0, val)

    acc = jnp.zeros((8, 128), F32)
    for quarter in (1, 2, 3, 0):
        acc = y_end(quarter, acc)
    sqs[0] = acc

    def sum_over(peers, src, buf, ssem, rsem):
        copies = [
            remote(src, buf.at[i], ssem.at[i], rsem.at[i], where) for i, where in enumerate(peers)
        ]
        for copy in copies:
            copy.start()
        return copies

    def take(copies, src, buf):
        for copy in copies:
            copy.wait_recv()
        acc = src[...]
        for i in range(len(copies)):
            acc = acc + buf[i]
        return acc

    qz = sum_over(z_peers, sqs.at[0], sqz, qz_send, qz_recv)
    outo_ref[:, lanes(mx * OB, OB)] = toto[mx]
    for quarter in range(1, 4):
        outq_ref[:, lanes(mx * QB + (quarter - 1) * OB, OB)] = totq[quarter - 1, mx]
    sqs[1] = take(qz, sqs.at[0], sqz)
    qp = sum_over(plane, sqs.at[1], sqp, qp_send, qp_recv)
    total = take(qp, sqs.at[1], sqp)
    total = jnp.sum(jnp.sum(total, axis=1, keepdims=True), axis=0, keepdims=True)
    factor_ref[...] = jnp.broadcast_to(lax.rsqrt(total / 16777216.0 + 1e-12), (8, 128))
    for quarter in range(4):
        for copy in o_copies(quarter):
            copy.wait_recv()
    def ring_sent(ring):
        for up in (True, False):
            for t in range(hops(up, ring)):
                ring_copy(up, t, ring).wait_send()

    for quarter in range(4):
        ring_sent(quarter)
        y_copy(quarter).wait_send()
        for copy in o_copies(quarter):
            copy.wait_send()

    @pl.when(sec < 4)
    def _():
        for c in range(1, NX):
            ring_sent(wide_ring(c))
            c_copy(c).wait_send()

    for copy in qz + qp:
        copy.wait_send()

    def finish(m, carry):
        for copy in act_copies(m, 0) + [relay_copy(m, 0)]:
            copy.wait_send()
        for k in (3, 4, 5):
            for copy in cot_copies(m, k):
                copy.wait_send()

        @pl.when(sec == 4)
        def _():
            for copy in act_copies(m, 1) + [relay_copy(m, 1)] + cot_copies(m, 2):
                copy.wait_send()

        @pl.when(sec < 3)
        def _():
            h_copy(m, 0).wait_send()
            h_copy(m, 1).wait_send()

        @pl.when(sec > 0)
        def _():
            g_copy(m).wait_send()

        return carry

    lax.fori_loop(0, 2, finish, 0)

    @pl.when(s0 == 1)
    def _():
        swap_mod().wait_send()
        swap_noise().wait_send()


def run_step(h0, mod, noise, w_qkv, w_out, head):
    shape = jax.ShapeDtypeStruct
    dma = pltpu.SemaphoreType.DMA
    vmem = pltpu.VMEM
    rows = NX * 2 * SEQ
    return pl.pallas_call(
        step_kernel,
        out_shape=(shape((16, 3 * D), F32), shape((16, D), F32), shape((8, 128), F32)),
        in_specs=[VMEM, VMEM, VMEM, ANY, ANY, VMEM],
        out_specs=[VMEM] * 3,
        scratch_shapes=[
            vmem((D, 3 * D), BF16),
            vmem((D, D), BF16),
            vmem((3 * D, D), BF16),
            vmem((D, D), BF16),
            vmem((rows, D), BF16),
            vmem((rows, D), BF16),
            vmem((rows, QB), BF16),
            vmem((rows, OB), BF16),
            vmem((8, NZ, 16, rows), BF16),
            vmem((8, NZ, 16, rows), BF16),
            vmem((2, SEQ, D), BF16),
            vmem((2, SEQ, D), BF16),
            vmem((2, SEQ, D), BF16),
            vmem((2, SEQ, D), BF16),
            vmem((2, SEQ, 3 * D), BF16),
            vmem((2, HEADS // 2, 2 * SEQ, SEQ), F32),
            vmem((2, SEQ, 128), F32),
            vmem((2, SEQ, D), BF16),
            vmem((2, SEQ, D), BF16),
            vmem((2, SEQ, 3 * D), BF16),
            vmem((2, SEQ, D), BF16),
            vmem((SEQ, D), BF16),
            vmem((SEQ, D), BF16),
            vmem((8, 3 * D), F32),
            vmem((2, 4, SEQ), BF16),
            vmem((28, 128, OB), BF16),
            vmem((28, 128, OB), BF16),
            vmem((28, 128, OB), BF16),
            vmem((28, 128, OB), BF16),
            vmem((NX, 128, OB), F32),
            vmem((NX, 128, OB), BF16),
            vmem((NX - 1, 128, OB), BF16),
            vmem((7, 8, NZ, 16, OB), F32),
            vmem((4, 2, NX * 16, OB), F32),
            vmem((4, NX * 16, OB), BF16),
            vmem((4, NX * 16, OB), BF16),
            vmem((3, NX, 16, OB), F32),
            vmem((NX, 16, OB), F32),
            vmem((2, 8, 128), F32),
            vmem((NZ - 1, 8, 128), F32),
            vmem((31, 8, 128), F32),
            dma((2, 2)), dma((2, 2)), dma((2,)), dma((2,)), dma((2,)), dma((2,)),
            dma((2, NX - 1, 6)), dma((2, NX - 1, 6)),
            dma((28,)), dma((28,)), dma((28,)), dma((28,)), dma((NX - 1,)), dma((NX - 1,)),
            dma((4,)), dma((4,)),
            dma((4, NX - 1)), dma((4, NX - 1)),
            dma((NZ - 1,)), dma((NZ - 1,)), dma((31,)), dma((31,)),
            dma((2,)),
        ],
        compiler_params=pltpu.CompilerParams(
            collective_id=0, has_side_effects=True, vmem_limit_bytes=62 * 2**20
        ),
        name="step",
    )(h0, mod, noise, w_qkv, w_out, head)


def optimizer_kernel(gq, go, factor_ref, mq, mo, vq, vo, uq, uo, nmq, nmo, nvq, nvo):
    factor = factor_ref[0:1, 0:1]
    for g, m, v, u, nm, nv in ((gq, mq, vq, uq, nmq, nvq), (go, mo, vo, uo, nmo, nvo)):
        normalized = g[...] * factor
        moment = 0.9 * m[0] + 0.1 * normalized
        second = 0.99 * v[0] + 0.01 * normalized * normalized
        u[0] = moment / (jnp.sqrt(second) + 1e-08)
        nm[0] = moment
        nv[0] = second


def optimizer(gq, go, factor, mq, mo, vq, vo):
    shape = jax.ShapeDtypeStruct
    big, small = shape((1, 16, 3 * D), F32), shape((1, 16, D), F32)
    return pl.pallas_call(
        optimizer_kernel,
        out_shape=(big, small, big, small, big, small),
        in_specs=[VMEM] * 7,
        out_specs=[VMEM] * 6,
        name="optimizer",
    )(gq, go, factor, mq, mo, vq, vo)


def local(
    latents,
    noise,
    timesteps,
    cameras,
    embed_in,
    camera_table,
    w_mod,
    w_qkv,
    w_out,
    head_out,
    moment_qkv,
    moment_out,
    second_qkv,
    second_out,
):
    time_emb = time_embed(timesteps, w_mod.shape[1])
    time_rows = jnp.pad(time_emb, ((0, 6), (0, 0)))
    mod = jnp.dot(time_rows, w_mod[0], preferred_element_type=jnp.float32)
    h0 = jax.vmap(embed_sample, in_axes=(0, 0, 0, 0, None, None))(
        latents, noise, timesteps, cameras, embed_in, camera_table
    )
    qkv_rows, out_rows, factors = run_step(h0, mod, noise, w_qkv[0], w_out[0], head_out)
    return optimizer(
        qkv_rows, out_rows, factors, moment_qkv, moment_out, second_qkv, second_out
    )


def solution(mesh):
    torus = Mesh(
        mesh.devices.reshape(2, 2, 2, 4, 8), ("section_0", "section_1", "dp_0", "dp_1", "dp_2")
    )
    return jax.shard_map(
        local,
        mesh=torus,
        in_specs=(
            P(DP, None, None),
            P(DP, None, None),
            P(DP),
            P(DP, None),
            P(),
            P(),
            P(SECTION, None, None),
            P(SECTION, None, None),
            P(SECTION, None, None),
            P(),
            P(SECTION, DP, None),
            P(SECTION, DP, None),
            P(SECTION, DP, None),
            P(SECTION, DP, None),
        ),
        out_specs=(
            P(SECTION, DP, None),
            P(SECTION, DP, None),
            P(SECTION, DP, None),
            P(SECTION, DP, None),
            P(SECTION, DP, None),
            P(SECTION, DP, None),
        ),
        check_vma=False,
    )
```
